32 devices in a mesh: blk: 8 (over y, x, core), uly: 4 (over z).
Axes of the slice: x: 2, y: 2, z: 4, core: 2. Of those that a mesh axis runs over, the one named last changes fastest.
Arguments:
- queries: bfloat16 [4096, 4096], P(('blk', 'uly')), may hold values from -100 to 100
- keys: bfloat16 [4096, 512], P(('blk', 'uly')), may hold values from -6 to 6
- values: bfloat16 [4096, 512], P(('blk', 'uly')), may hold values from -6 to 6
- segments: int32 [4096], P(('blk', 'uly')), may hold values from 0 to 7, never falling along the last dimension, each value on 1 to 2048 neighbouring positions
Outputs:
- attended: bfloat16 [4096, 4096], P(('blk', 'uly'))
The draws below stay inside these ranges and needn't reach their ends.
Inputs may be any that keep to these rules, and one draw needn't show every extreme that they name: `segments`: document numbers never fall along the sequence; each document holds 1 to 2048 positions.
All inputs are finite; a program needn't handle non-finite values.
Results may differ from the reference program's by a relative error of at most 0.0039.
Values may be sent and summed in bfloat16 or wider, within the bound.
No kernel may reach another device: no remote copies, remote signals or barrier semaphores. Data moves between devices by JAX's collectives and lax.ppermute only.
A program may use at most 64 MiB of HBM per device.

```python
import math
import jax
import jax.numpy as jnp
import numpy as np
from jax import lax

QUERY_HEADS = 32
KEY_VALUE_HEADS = 4
HEAD_SIZE = 128
NDOC = 8
SEQUENCE_LENGTH = 4096


def shared_pair(key):
    base_offset = jax.random.fold_in(key, 7)
    key_subset = jnp.clip(jax.random.normal(jax.random.fold_in(base_offset, 1), (SEQUENCE_LENGTH, KEY_VALUE_HEADS * HEAD_SIZE), jnp.float32), -6.0, 6.0)
    queryset = jnp.clip(jax.random.normal(jax.random.fold_in(base_offset, 2), (SEQUENCE_LENGTH, QUERY_HEADS * HEAD_SIZE), jnp.float32), -6.0, 6.0)
    return (queryset, key_subset)


def draw_queries(key, part):
    return shared_pair(key)[0].astype(jnp.bfloat16)


def draw_keys(key, part):
    return shared_pair(key)[1].astype(jnp.bfloat16)


def levels(stream_key, shape, shards, least, top_value):
    def one(axis_at, shards_of):
        draws = jax.random.uniform(jax.random.fold_in(jax.random.fold_in(stream_key, 6), axis_at), (shards_of,), jnp.float32, least / len(shards), top_value / len(shards))
        return jnp.repeat(jnp.exp(draws), shape[axis_at] // shards_of).reshape((-1,) + (1,) * (len(shape) - axis_at - 1))

    loudness = one(*shards[0])
    for cut in shards[1:]:
        loudness = loudness * one(*cut)
    return loudness


def split_up(number_of, total, reach, lean):
    loads = [(1 << 20) // math.isqrt(standing ** lean) + 1 for standing in range(2, number_of + 1)]
    spare, given = total - reach - (number_of - 1), [1] * (number_of - 1)
    while spare > 0:
        movable = [i for i in range(number_of - 1) if given[i] < reach]
        pool, budget = sum([loads[i] for i in movable]), spare
        for i in movable:
            addition = min(reach - given[i], max(1, budget * loads[i] // pool), spare)
            given[i] = given[i] + addition
            spare = spare - addition
    return np.array([reach] + given)


def uneven(key, amount, total, bound, slope):
    if amount == 2:
        one = jax.random.randint(key, (), max(1, total - bound), min(bound, total - 1) + 1)
        return jnp.stack([one, total - one])
    tallies = jnp.asarray(split_up(amount, total, bound, slope), jnp.int32)
    twos = (amount - 1) // 2
    source_of, sink = tallies[1:1 + 2 * twos:2], tallies[2:2 + 2 * twos:2]
    room = jnp.minimum(source_of - 1, bound - sink)
    moved = jax.random.randint(jax.random.fold_in(key, 1), (twos,), 0, 1 << 20) % (room + 1)
    tallies = tallies.at[1:1 + 2 * twos:2].set(source_of - moved).at[2:2 + 2 * twos:2].set(sink + moved)
    return tallies[jax.random.permutation(jax.random.fold_in(key, 2), amount)]


def centred(own_key, extent, deviation, most, cuts=(), held_as=jnp.bfloat16):
    entries = jax.random.normal(own_key, extent, jnp.float32) * deviation
    if len(cuts) > 0:
        entries = levels(own_key, extent, cuts, -0.22, 0.18) * entries
    return jnp.clip(entries, min=-most, max=most).astype(held_as)


def setup_inputs(seed: int = 0) -> dict:
    key_list = jax.random.split(jax.random.key(seed), 5)
    queries = draw_queries(jax.random.fold_in(key_list[4], 71), 0)
    keys = draw_keys(jax.random.fold_in(key_list[4], 71), 0)
    values = centred(key_list[2], (SEQUENCE_LENGTH, KEY_VALUE_HEADS * HEAD_SIZE), 1.0, 6.0, ((0, 32),))
    segments = jnp.searchsorted(jnp.cumsum(uneven(key_list[3], NDOC, SEQUENCE_LENGTH, SEQUENCE_LENGTH // 2, 2)), jnp.arange(SEQUENCE_LENGTH), side="right").astype(jnp.int32)
    return {"queries": queries, "keys": keys, "values": values, "segments": segments}


def reference(queries, keys, values, segments):
    span_length = queries.shape[0]
    head_groups = QUERY_HEADS // KEY_VALUE_HEADS
    block = min(512, span_length)
    count = span_length // block
    scale = HEAD_SIZE ** -0.5
    query_rows = queries.reshape(span_length, KEY_VALUE_HEADS, head_groups, HEAD_SIZE)
    key_rows = keys.reshape(span_length, KEY_VALUE_HEADS, HEAD_SIZE)
    value_rows = values.reshape(span_length, KEY_VALUE_HEADS, HEAD_SIZE)
    places = jnp.arange(span_length, dtype=jnp.int32)

    def single_head(head):
        qhead = query_rows[:, head]
        khead = key_rows[:, head].astype(jnp.float32)
        vhead = value_rows[:, head].astype(jnp.float32)

        def one_block(index):
            first = (index * block).astype(jnp.int32)
            qblk = lax.dynamic_slice_in_dim(qhead, first, block, 0).astype(jnp.float32)
            qpos = first + jnp.arange(block, dtype=jnp.int32)
            qseg = lax.dynamic_slice_in_dim(segments, first, block, 0)
            scores = jnp.einsum("qgd,kd->gqk", qblk, khead) * scale
            allowed = (places[None, :] <= qpos[:, None]) & (segments[None, :] == qseg[:, None])
            scores = jnp.where(allowed[None], scores, -1e30)
            top = jnp.max(scores, axis=-1, keepdims=True)
            probs = jnp.where(allowed[None], jnp.exp(scores - top), 0.0)
            total = jnp.sum(probs, axis=-1)
            rounded = lax.optimization_barrier(probs.astype(jnp.bfloat16)).astype(jnp.float32)
            summed = jnp.einsum("gqk,kd->qgd", rounded, vhead)
            return summed / jnp.transpose(total)[:, :, None]

        return lax.map(one_block, jnp.arange(count, dtype=jnp.int32))

    final_output = lax.map(single_head, jnp.arange(KEY_VALUE_HEADS, dtype=jnp.int32))
    final_output = jnp.transpose(final_output, (1, 2, 0, 3, 4)).reshape(span_length, QUERY_HEADS * HEAD_SIZE)
    return final_output.astype(jnp.bfloat16)
```

```python
import functools

import jax
import jax.numpy as jnp
from jax import lax
from jax.experimental import pallas as pl
from jax.experimental.pallas import tpu as pltpu
from jax.sharding import Mesh
from jax.sharding import PartitionSpec as P

HEAD_SIZE = 128
LOG2E = 1.4426950408889634
LOW = -1e30


def attend(where, q_ref, own_ref, mate_ref, out_ref, s_ref, p_ref, m_ref, l_ref, acc_ref, *, rows, layers, split):
    groups, _, width = q_ref.shape
    per = width // HEAD_SIZE
    sources = own_ref.shape[0]
    block = layers * rows
    scale = HEAD_SIZE ** -0.5 * LOG2E
    chip0, core, layer = where[0], where[1], where[2]

    counts = jnp.zeros((8, HEAD_SIZE), jnp.float32)
    for ref in (own_ref, mate_ref):
        for i in range(sources):
            counts = counts + ref[i, 2 * rows :, :].astype(jnp.float32)
    ends = counts[:1]

    part = per // split
    for g in range(groups):
        blk = (chip0 + g) * 2 + core
        first = (blk * layers + layer) * rows
        place = first + lax.broadcasted_iota(jnp.int32, (rows, 1), 0)
        placef = place.astype(jnp.float32)
        start = jnp.max(jnp.where(ends <= placef, ends, 0.0), axis=1, keepdims=True).astype(jnp.int32)
        low = jnp.min(start)
        low_blk = low // block
        m_ref[...] = jnp.full(m_ref.shape, LOW, jnp.float32)
        l_ref[...] = jnp.zeros(l_ref.shape, jnp.float32)
        acc_ref[...] = jnp.zeros(acc_ref.shape, jnp.float32)

        def step(ref, chip, parity):
            base = (chip * 2 + parity) * block
            k = jnp.concatenate([ref[chip * layers + z, :rows, :] for z in range(layers)], axis=0)
            v = jnp.concatenate([ref[chip * layers + z, rows : 2 * rows, :] for z in range(layers)], axis=0)
            key = base + lax.broadcasted_iota(jnp.int32, (rows, block), 1)
            bias = jnp.where((key <= place) & (key >= start), 0.0, LOW)
            for h0 in range(0, per, part):
                q = jnp.concatenate(
                    [q_ref[g, :, h * HEAD_SIZE : (h + 1) * HEAD_SIZE] for h in range(h0, h0 + part)], axis=0
                )
                s = lax.dot_general(q, k, (((1,), (1,)), ((), ())), preferred_element_type=jnp.float32)
                ps = []
                factors = []
                for i in range(part):
                    r = pl.ds((h0 + i) * rows, rows)
                    x = s[i * rows : (i + 1) * rows] * scale + bias
                    old = m_ref[r, :]
                    top = jnp.maximum(old, jnp.max(x, axis=1, keepdims=True))
                    p = jnp.exp2(x - top[:, :1])
                    factor = jnp.exp2(old - top)
                    m_ref[r, :] = top
                    l_ref[r, :] = l_ref[r, :] * factor + jnp.sum(p, axis=1, keepdims=True)
                    ps.append(p.astype(jnp.bfloat16))
                    factors.append(factor)
                pv = lax.dot_general(
                    jnp.concatenate(ps, axis=0), v, (((1,), (0,)), ((), ())), preferred_element_type=jnp.float32
                )
                r = pl.ds(h0 * rows, part * rows)
                acc_ref[r, :] = acc_ref[r, :] * jnp.concatenate(factors, axis=0) + pv

        @pl.loop((low_blk - core + 1) // 2, chip0 + g + 1)
        def _(chip):
            step(own_ref, chip, core)

        other = 1 - core

        @pl.loop((low_blk - other + 1) // 2, (blk - other) // 2 + 1)
        def _(chip):
            step(mate_ref, chip, other)

        for h in range(per):
            r = pl.ds(h * rows, rows)
            out_ref[g, :, h * HEAD_SIZE : (h + 1) * HEAD_SIZE] = (acc_ref[r, :] / l_ref[r, :]).astype(out_ref.dtype)


def local(queries, keys, values, segments, *, outer, groups, layers):
    rows = queries.shape[0]
    per_head = queries.shape[1] // groups
    per = per_head // HEAD_SIZE
    members = outer * groups * layers
    below = (segments[:, None] < jnp.arange(HEAD_SIZE, dtype=jnp.int32)[None, :]).astype(jnp.float32)
    counts = jnp.broadcast_to(jnp.sum(below, axis=0)[None, :], (8, HEAD_SIZE)).astype(jnp.bfloat16)

    q = lax.all_to_all(
        queries.reshape(rows, groups, per_head).swapaxes(0, 1), "group", split_axis=0, concat_axis=0, tiled=True
    )
    kv = jnp.concatenate(
        [
            keys.reshape(rows, groups, HEAD_SIZE).swapaxes(0, 1),
            values.reshape(rows, groups, HEAD_SIZE).swapaxes(0, 1),
            jnp.broadcast_to(counts[None], (groups, 8, HEAD_SIZE)),
        ],
        axis=1,
    )
    piece = kv.shape[1]
    sent = jnp.broadcast_to(kv[None, :, None], (outer, groups, layers, piece, HEAD_SIZE))
    own = lax.all_to_all(
        sent.reshape(members, piece, HEAD_SIZE), ("outer", "group", "uly"), split_axis=0, concat_axis=0, tiled=True
    )
    mate = lax.ppermute(own, "core", [(0, 1), (1, 0)])
    where = jnp.stack(
        [lax.axis_index("outer") * groups, lax.axis_index("core"), lax.axis_index("uly")]
    ).astype(jnp.int32)
    block = layers * rows
    vmem = pl.BlockSpec(memory_space=pltpu.VMEM)
    out = pl.pallas_call(
        functools.partial(attend, rows=rows, layers=layers, split=2),
        out_shape=jax.ShapeDtypeStruct((groups, rows, per_head), jnp.bfloat16),
        in_specs=[pl.BlockSpec(memory_space=pltpu.SMEM), vmem, vmem, vmem],
        out_specs=vmem,
        scratch_shapes=[
            pltpu.VMEM((8, HEAD_SIZE), jnp.float32),
            pltpu.VMEM((16, HEAD_SIZE), jnp.bfloat16),
            pltpu.VMEM((per * rows, HEAD_SIZE), jnp.float32),
            pltpu.VMEM((per * rows, HEAD_SIZE), jnp.float32),
            pltpu.VMEM((per * rows, HEAD_SIZE), jnp.float32),
        ],
        name="attend",
    )(where, q, own, mate)
    back = lax.all_to_all(out, "group", split_axis=0, concat_axis=0, tiled=True)
    return back.swapaxes(0, 1).reshape(rows, groups * per_head)


def solution(mesh):
    blocks, layers = mesh.shape["blk"], mesh.shape["uly"]

    def run(queries, keys, values, segments):
        groups = keys.shape[1] // HEAD_SIZE
        outer = blocks // 2 // groups
        fine = Mesh(mesh.devices.reshape(outer, groups, 2, layers), ("outer", "group", "core", "uly"))
        axes = ("outer", "group", "core", "uly")
        body = functools.partial(local, outer=outer, groups=groups, layers=layers)
        return jax.shard_map(
            body, mesh=fine, in_specs=(P(axes), P(axes), P(axes), P(axes)), out_specs=P(axes), check_vma=False
        )(queries, keys, values, segments)

    return run
```

```python
import functools

import jax
import jax.numpy as jnp
from jax import lax
from jax.experimental import pallas as pl
from jax.experimental.pallas import tpu as pltpu
from jax.sharding import Mesh
from jax.sharding import PartitionSpec as P


HEAD_SIZE = 128
DOCUMENTS = 8
LOG2E = 1.4426950408889634
LOW = -1e30
AXES = ("outer", "group", "core", "uly")
VMEM = pl.BlockSpec(memory_space=pltpu.VMEM)
HBM = pl.BlockSpec(memory_space=pl.ANY)


def pack(q_ref, k_ref, v_ref, seg_ref, kv_ref, *rest, outer, groups, layers):
    q_out, sems = rest[:groups], rest[groups]
    rows, width = q_out[0].shape
    mine = lax.axis_index("group")
    copies = []
    for i in range(groups):
        start = pl.multiple_of((mine ^ i) * width, width)
        copies.append(pltpu.make_async_copy(q_ref.at[:, pl.ds(start, width)], q_out[i], sems.at[i]))
        copies[-1].start()
    number = lax.broadcasted_iota(jnp.int32, (DOCUMENTS, rows), 0)
    below = jnp.where(seg_ref[...] < number, 1.0, 0.0)
    counts = jnp.broadcast_to(jnp.sum(below, axis=1, keepdims=True), (DOCUMENTS, HEAD_SIZE)).astype(jnp.bfloat16)
    for g in range(groups):
        cut = slice(g * HEAD_SIZE, (g + 1) * HEAD_SIZE)
        k, v = k_ref[:, cut], v_ref[:, cut]
        for o in range(outer):
            for z in range(layers):
                to = (o * groups + g) * layers + z
                kv_ref[to, :rows, :] = k
                kv_ref[to, rows : 2 * rows, :] = v
                kv_ref[to, 2 * rows :, :] = counts
    for copy in copies:
        copy.wait()


def attend(q_ref, own_ref, mate_ref, out_ref, m_ref, l_ref, acc_ref, *, index, rows, groups, layers, split):
    width = q_ref.shape[1]
    per = width // HEAD_SIZE
    sources = own_ref.shape[0]
    block = layers * rows
    scale = HEAD_SIZE ** -0.5 * LOG2E
    core, layer = lax.axis_index("core"), lax.axis_index("uly")
    home = lax.axis_index("outer") * groups + (lax.axis_index("group") ^ index)

    ends = jnp.zeros((DOCUMENTS, HEAD_SIZE), jnp.float32)
    for ref in (own_ref, mate_ref):
        for i in range(sources):
            ends = ends + ref[i, 2 * rows :, :].astype(jnp.float32)
    blk = home * 2 + core
    first = (blk * layers + layer) * rows
    place = first + lax.broadcasted_iota(jnp.int32, (rows, HEAD_SIZE), 0)
    start = jnp.zeros((rows, HEAD_SIZE), jnp.int32)
    for d in range(DOCUMENTS):
        end = jnp.broadcast_to(ends[d : d + 1], (rows, HEAD_SIZE)).astype(jnp.int32)
        start = jnp.where(end <= place, jnp.maximum(start, end), start)
    place, start = place[:, :1], start[:, :1]
    low_blk = jnp.min(start) // block
    m_ref[...] = jnp.full(m_ref.shape, LOW, jnp.float32)
    l_ref[...] = jnp.zeros(l_ref.shape, jnp.float32)
    acc_ref[...] = jnp.zeros(acc_ref.shape, jnp.float32)
    part = per // split

    def step(ref, chip, parity):
        base = (chip * 2 + parity) * block
        k = jnp.concatenate([ref[chip * layers + z, :rows, :] for z in range(layers)], axis=0)
        v = jnp.concatenate([ref[chip * layers + z, rows : 2 * rows, :] for z in range(layers)], axis=0)
        key = base + lax.broadcasted_iota(jnp.int32, (rows, block), 1)
        bias = jnp.where((key <= place) & (key >= start), 0.0, LOW)
        for h0 in range(0, per, part):
            q = jnp.concatenate([q_ref[:, h * HEAD_SIZE : (h + 1) * HEAD_SIZE] for h in range(h0, h0 + part)], axis=0)
            s = lax.dot_general(q, k, (((1,), (1,)), ((), ())), preferred_element_type=jnp.float32)
            ps = []
            factors = []
            for i in range(part):
                r = pl.ds((h0 + i) * rows, rows)
                x = s[i * rows : (i + 1) * rows] * scale + bias
                old = m_ref[r, :]
                top = jnp.maximum(old, jnp.max(x, axis=1, keepdims=True))
                p = jnp.exp2(x - top[:, :1])
                factor = jnp.exp2(old - top)
                m_ref[r, :] = top
                l_ref[r, :] = l_ref[r, :] * factor + jnp.sum(p, axis=1, keepdims=True)
                ps.append(p.astype(jnp.bfloat16))
                factors.append(factor)
            pv = lax.dot_general(
                jnp.concatenate(ps, axis=0), v, (((1,), (0,)), ((), ())), preferred_element_type=jnp.float32
            )
            r = pl.ds(h0 * rows, part * rows)
            acc_ref[r, :] = acc_ref[r, :] * jnp.concatenate(factors, axis=0) + pv

    @pl.loop((low_blk - core + 1) // 2, home + 1)
    def _(chip):
        step(own_ref, chip, core)

    other = 1 - core

    @pl.loop((low_blk - other + 1) // 2, home + core)
    def _(chip):
        step(mate_ref, chip, other)

    for h in range(per):
        r = pl.ds(h * rows, rows)
        out_ref[:, h * HEAD_SIZE : (h + 1) * HEAD_SIZE] = (acc_ref[r, :] / l_ref[r, :]).astype(out_ref.dtype)


def place(*refs, groups):
    pieces, out_ref, sems = refs[:groups], refs[groups], refs[groups + 1]
    width = pieces[0].shape[1]
    mine = lax.axis_index("group")
    copies = []
    for i in range(groups):
        start = pl.multiple_of((mine ^ i) * width, width)
        copies.append(pltpu.make_async_copy(pieces[i], out_ref.at[:, pl.ds(start, width)], sems.at[i]))
        copies[-1].start()
    for copy in copies:
        copy.wait()


def local(queries, keys, values, segments, *, outer, groups, layers):
    rows = queries.shape[0]
    width = queries.shape[1] // groups
    per = width // HEAD_SIZE
    members = outer * groups * layers
    sizes = dict(groups=groups, layers=layers)
    piece = jax.ShapeDtypeStruct((rows, width), jnp.bfloat16)
    kv, *q = pl.pallas_call(
        functools.partial(pack, outer=outer, **sizes),
        out_shape=[jax.ShapeDtypeStruct((members, 2 * rows + DOCUMENTS, HEAD_SIZE), jnp.bfloat16)] + [piece] * groups,
        in_specs=[HBM, VMEM, VMEM, VMEM],
        out_specs=[VMEM] * (groups + 1),
        scratch_shapes=[pltpu.SemaphoreType.DMA((groups,))],
        compiler_params=pltpu.CompilerParams(vmem_limit_bytes=16 << 20),
        name="pack",
    )(queries, keys, values, segments.reshape(1, rows))
    own = lax.all_to_all(kv, ("outer", "group", "uly"), split_axis=0, concat_axis=0, tiled=True)

    def swap(x, i):
        return lax.ppermute(x, "group", [(g, g ^ i) for g in range(groups)])

    order = list(range(groups - 1, 0, -1))
    for i in order:
        q[i] = swap(q[i], i)
    own, *q[1:] = lax.optimization_barrier((own, *q[1:]))
    mate = lax.ppermute(own, "core", [(0, 1), (1, 0)])
    out = [None] * groups
    before = None
    for i in order + [0]:
        if before is not None:
            q[i], before = lax.optimization_barrier((q[i], before))
        call = pl.pallas_call(
            functools.partial(attend, index=i, rows=rows, split=2, **sizes),
            out_shape=piece,
            in_specs=[VMEM] * 3,
            out_specs=VMEM,
            scratch_shapes=[pltpu.VMEM((per * rows, HEAD_SIZE), jnp.float32)] * 3,
            compiler_params=pltpu.CompilerParams(vmem_limit_bytes=24 << 20),
            cost_estimate=pl.CostEstimate(
                flops=2 * rows * width * members * rows, transcendentals=0, bytes_accessed=4 * rows * width
            ),
            name="attend",
        )
        before = out[i] = call(q[i], own, mate)
        if i:
            out[i] = swap(out[i], i)
    return pl.pallas_call(
        functools.partial(place, groups=groups),
        out_shape=jax.ShapeDtypeStruct(queries.shape, jnp.bfloat16),
        in_specs=[VMEM] * groups,
        out_specs=HBM,
        scratch_shapes=[pltpu.SemaphoreType.DMA((groups,))],
        compiler_params=pltpu.CompilerParams(vmem_limit_bytes=8 << 20),
        name="place",
    )(*out)


def solution(mesh):
    blocks, layers = mesh.shape["blk"], mesh.shape["uly"]

    def run(queries, keys, values, segments):
        groups = keys.shape[1] // HEAD_SIZE
        outer = blocks // 2 // groups
        fine = Mesh(mesh.devices.reshape(outer, groups, 2, layers), AXES)

        def body(*args):
            return local(*args, outer=outer, groups=groups, layers=layers)

        spec = P(AXES)
        step = jax.shard_map(body, mesh=fine, in_specs=(spec,) * 4, out_specs=spec, check_vma=False)
        return step(queries, keys, values, segments)

    return run
```

```python
import functools

import jax
import jax.numpy as jnp
from jax import lax
from jax.experimental import pallas as pl
from jax.experimental.pallas import tpu as pltpu
from jax.sharding import Mesh
from jax.sharding import PartitionSpec as P


HEAD_SIZE = 128
DOCUMENTS = 8
LOG2E = 1.4426950408889634
LOW = -1e30
AXES = ("outer", "group", "core", "uly")
VMEM = pl.BlockSpec(memory_space=pltpu.VMEM)
HBM = pl.BlockSpec(memory_space=pltpu.HBM)


def pack(q_ref, k_ref, v_ref, seg_ref, *rest, groups):
    kv_out, q_out, (k_buf, v_buf, seg_buf, sems) = rest[:groups], rest[groups : 2 * groups], rest[2 * groups :]
    rows, width = q_out[0].shape
    mine = lax.axis_index("group")
    first = [
        pltpu.make_async_copy(seg_ref, seg_buf, sems.at[groups]),
        pltpu.make_async_copy(k_ref, k_buf, sems.at[groups + 1]),
        pltpu.make_async_copy(v_ref, v_buf, sems.at[groups + 2]),
    ]
    later = []
    for i in range(groups):
        start = pl.multiple_of((mine ^ i) * width, width)
        later.append(pltpu.make_async_copy(q_ref.at[:, pl.ds(start, width)], q_out[i], sems.at[i]))
    for copy in first + later:
        copy.start()
    first[0].wait()
    number = lax.broadcasted_iota(jnp.int32, (DOCUMENTS, rows), 0)
    below = jnp.where(seg_buf[...] < number, 1.0, 0.0)
    counts = jnp.broadcast_to(jnp.sum(below, axis=1, keepdims=True), (DOCUMENTS, HEAD_SIZE)).astype(jnp.bfloat16)
    first[1].wait()
    first[2].wait()
    for i in range(groups):
        cut = pl.ds(pl.multiple_of((mine ^ i) * HEAD_SIZE, HEAD_SIZE), HEAD_SIZE)
        kv_out[i][:rows, :] = k_buf[:, cut]
        kv_out[i][rows : 2 * rows, :] = v_buf[:, cut]
        kv_out[i][2 * rows :, :] = counts
    for copy in later:
        copy.wait()


def merge(*refs, groups):
    pieces, out_ref = refs[:groups], refs[groups]
    mine = lax.axis_index("group")
    for i in range(groups):
        out_ref[mine ^ i] = pieces[i][...]


def attend(*refs, index, turns, rows, groups, layers, split, final):
    count = len(turns)
    q_ref, home_ref = refs[:2]
    own, mate = refs[2 : 2 + count], refs[2 + count : 2 + 2 * count]
    rest = refs[2 + 2 * count :]
    if final:
        state, out_ref, held = rest[:3], rest[3], rest[4:]
    else:
        held = rest
    m_ref, l_ref, acc_ref = held
    per = q_ref.shape[1] // HEAD_SIZE
    chips = own[0].shape[0]
    scale = HEAD_SIZE ** -0.5 * LOG2E
    core, layer = lax.axis_index("core"), lax.axis_index("uly")
    home = lax.axis_index("outer") * groups + (lax.axis_index("group") ^ index)
    shape = (rows, HEAD_SIZE)
    lane = lax.broadcasted_iota(jnp.int32, (DOCUMENTS, HEAD_SIZE), 1).astype(jnp.float32)
    number = lax.broadcasted_iota(jnp.int32, (DOCUMENTS, HEAD_SIZE), 0).astype(jnp.float32)

    def counts(ref, chip):
        return ref[chip, 2 * rows :, :].astype(jnp.float32)

    mine = counts(home_ref, home)
    local_row = lax.broadcasted_iota(jnp.int32, shape, 0).astype(jnp.float32)
    row_doc = jnp.zeros(shape, jnp.float32)
    for d in range(DOCUMENTS):
        row_doc = row_doc + jnp.where(jnp.broadcast_to(mine[d : d + 1], shape) <= local_row, 1.0, 0.0)
    place = ((home * 2 + core) * layers + layer) * rows + lax.broadcasted_iota(jnp.int32, shape, 0)
    earliest = row_doc[:1] - 1.0

    def skipped(tiles):
        gone = jnp.zeros((1, HEAD_SIZE), jnp.float32)
        for chip in range(chips):
            least = None
            for ref in tiles:
                held_below = jnp.sum(jnp.where(number == earliest, counts(ref, chip), 0.0), axis=0, keepdims=True)
                least = held_below if least is None else jnp.minimum(least, held_below)
            gone = gone + jnp.where(least >= rows, 1.0, 0.0)
        return jnp.max(gone).astype(jnp.int32)

    if final:
        for into, ref in zip(held, state):
            into[...] = ref[...]
    else:
        m_ref[...] = jnp.full(m_ref.shape, LOW, jnp.float32)
        l_ref[...] = jnp.zeros(l_ref.shape, jnp.float32)
        acc_ref[...] = jnp.zeros(acc_ref.shape, jnp.float32)
    part = per // split

    def step(tiles, chip, parity):
        k = jnp.concatenate([ref[chip, :rows, :] for ref in tiles], axis=0)
        v = jnp.concatenate([ref[chip, rows : 2 * rows, :] for ref in tiles], axis=0)
        bias = []
        for turn, ref in zip(turns, tiles):
            base = ((chip * 2 + parity) * layers + (layer ^ turn)) * rows
            key_doc = jnp.sum(jnp.where(counts(ref, chip) <= lane, 1.0, 0.0), axis=0, keepdims=True)
            key = base + lax.broadcasted_iota(jnp.int32, shape, 1)
            bias.append(jnp.where((key <= place) & (row_doc == key_doc), 0.0, LOW))
        for h0 in range(0, per, part):
            q = jnp.concatenate([q_ref[:, h * HEAD_SIZE : (h + 1) * HEAD_SIZE] for h in range(h0, h0 + part)], axis=0)
            s = lax.dot_general(q, k, (((1,), (1,)), ((), ())), preferred_element_type=jnp.float32)
            ps = []
            factors = []
            for i in range(part):
                r = pl.ds((h0 + i) * rows, rows)
                xs = [s[i * rows : (i + 1) * rows, c * rows : (c + 1) * rows] + bias[c] for c in range(count)]
                old = m_ref[r, :]
                top = jnp.maximum(old, jnp.max(functools.reduce(jnp.maximum, xs), axis=1, keepdims=True))
                m_ref[r, :] = top
                shift = top * scale
                p = [jnp.exp2(x * scale - shift) for x in xs]
                factor = jnp.exp2(old * scale - shift)
                l_ref[r, :] = l_ref[r, :] * factor + functools.reduce(jnp.add, p)
                ps.append(jnp.concatenate([y.astype(jnp.bfloat16) for y in p], axis=1))
                factors.append(factor)
            pv = lax.dot_general(
                jnp.concatenate(ps, axis=0), v, (((1,), (0,)), ((), ())), preferred_element_type=jnp.float32
            )
            r = pl.ds(h0 * rows, part * rows)
            acc_ref[r, :] = acc_ref[r, :] * jnp.concatenate(factors, axis=0) + pv

    @pl.loop(skipped(own), home + 1)
    def _(chip):
        step(own, chip, core)

    @pl.loop(skipped(mate), home + core)
    def _(chip):
        step(mate, chip, 1 - core)

    if final:
        for h in range(per):
            r = pl.ds(h * rows, rows)
            total = jnp.sum(l_ref[r, :], axis=1, keepdims=True)
            out_ref[:, h * HEAD_SIZE : (h + 1) * HEAD_SIZE] = (acc_ref[r, :] / total).astype(out_ref.dtype)


def place(*refs, groups):
    pieces, out_ref, sems = refs[:groups], refs[groups], refs[groups + 1]
    width = pieces[0].shape[1]
    mine = lax.axis_index("group")
    copies = []
    for i in range(groups):
        start = pl.multiple_of((mine ^ i) * width, width)
        copies.append(pltpu.make_async_copy(pieces[i], out_ref.at[:, pl.ds(start, width)], sems.at[i]))
        copies[-1].start()
    for copy in copies:
        copy.wait()


def limit(mib):
    return pltpu.CompilerParams(vmem_limit_bytes=mib << 20)


def local(queries, keys, values, segments, *, outer, groups, layers):
    rows = queries.shape[0]
    width = queries.shape[1] // groups
    per = width // HEAD_SIZE
    piece = jax.ShapeDtypeStruct((rows, width), jnp.bfloat16)
    one = jax.ShapeDtypeStruct((2 * rows + DOCUMENTS, HEAD_SIZE), jnp.bfloat16)
    made = pl.pallas_call(
        functools.partial(pack, groups=groups),
        out_shape=[one] * groups + [piece] * groups,
        in_specs=[HBM] * 4,
        out_specs=[VMEM] * (2 * groups),
        scratch_shapes=[
            pltpu.VMEM(keys.shape, jnp.bfloat16),
            pltpu.VMEM(values.shape, jnp.bfloat16),
            pltpu.VMEM((1, rows), jnp.int32),
            pltpu.SemaphoreType.DMA((groups + 3,)),
        ],
        compiler_params=limit(8),
        name="pack",
    )(*(pltpu.with_memory_space_constraint(x, pltpu.HBM) for x in (queries, keys, values, segments.reshape(1, rows))))
    kv, q = list(made[:groups]), list(made[groups:])

    def swap(x, axis, size, i):
        return lax.ppermute(x, axis, [(g, g ^ i) for g in range(size)])

    order = list(range(groups - 1, 0, -1))
    for i in order:
        kv[i] = swap(kv[i], "group", groups, i)
    for i in order:
        q[i] = swap(q[i], "group", groups, i)
    mine = pl.pallas_call(
        functools.partial(merge, groups=groups),
        out_shape=jax.ShapeDtypeStruct((groups, *one.shape), jnp.bfloat16),
        in_specs=[VMEM] * groups,
        out_specs=VMEM,
        compiler_params=limit(4),
        name="merge",
    )(*kv)
    if outer > 1:
        mine = lax.all_gather(mine, "outer", axis=0, tiled=True)
    own = [mine] + [swap(mine, "uly", layers, j) for j in range(1, layers)]
    mate = []
    for j in range(layers):
        mate.append(lax.ppermute(own[j], "core", [(0, 1), (1, 0)]))

    held = [jax.ShapeDtypeStruct((per * rows, HEAD_SIZE), jnp.float32)] * 3
    common = dict(rows=rows, groups=groups, layers=layers, split=2)
    near, far = list(range(layers // 2)), list(range(layers // 2, layers))

    def call(i, turns, final, *args):
        return pl.pallas_call(
            functools.partial(attend, index=i, turns=turns, final=final, **common),
            out_shape=piece if final else held,
            in_specs=[VMEM] * len(args),
            out_specs=VMEM if final else [VMEM] * 3,
            scratch_shapes=[pltpu.VMEM(x.shape, x.dtype) for x in held] if final else [],
            compiler_params=limit(16),
            name="attend",
        )(*args)

    states = [None] * groups
    last = None
    for i in order + [0]:
        if last is not None:
            q[i], last = lax.optimization_barrier((q[i], last))
        states[i] = call(i, near, False, q[i], own[0], *(own[j] for j in near), *(mate[j] for j in near))
        last = states[i][0]
    out = [None] * groups
    last = None
    for i in order + [0]:
        if last is not None:
            q[i], last = lax.optimization_barrier((q[i], last))
        last = call(i, far, True, q[i], own[0], *(own[j] for j in far), *(mate[j] for j in far), *states[i])
        out[i] = swap(last, "group", groups, i) if i else last
    return pl.pallas_call(
        functools.partial(place, groups=groups),
        out_shape=jax.ShapeDtypeStruct(queries.shape, jnp.bfloat16),
        in_specs=[VMEM] * groups,
        out_specs=HBM,
        scratch_shapes=[pltpu.SemaphoreType.DMA((groups,))],
        compiler_params=limit(4),
        name="place",
    )(*out)


def solution(mesh):
    blocks, layers = mesh.shape["blk"], mesh.shape["uly"]

    def run(queries, keys, values, segments):
        groups = keys.shape[1] // HEAD_SIZE
        outer = blocks // 2 // groups
        fine = Mesh(mesh.devices.reshape(outer, groups, 2, layers), AXES)

        def body(*args):
            return local(*args, outer=outer, groups=groups, layers=layers)

        spec = P(AXES)
        step = jax.shard_map(body, mesh=fine, in_specs=(spec,) * 4, out_specs=spec, check_vma=False)
        return step(queries, keys, values, segments)

    return run
```

```python
import functools

import jax
import jax.numpy as jnp
from jax import lax
from jax.experimental import pallas as pl
from jax.experimental.pallas import tpu as pltpu
from jax.sharding import Mesh
from jax.sharding import PartitionSpec as P


HEAD_SIZE = 128
DOCUMENTS = 8
LOG2E = 1.4426950408889634
LOW = -1e30
AXES = ("outer", "group", "core", "uly")
VMEM = pl.BlockSpec(memory_space=pltpu.VMEM)
HBM = pl.BlockSpec(memory_space=pltpu.HBM)


def pack(q_ref, k_ref, v_ref, seg_ref, *rest, groups):
    kv_out, q_out, (k_buf, v_buf, seg_buf, sems) = rest[:groups], rest[groups : 2 * groups], rest[2 * groups :]
    rows, width = q_out[0].shape
    mine = lax.axis_index("group")
    first = [
        pltpu.make_async_copy(seg_ref, seg_buf, sems.at[groups]),
        pltpu.make_async_copy(k_ref, k_buf, sems.at[groups + 1]),
        pltpu.make_async_copy(v_ref, v_buf, sems.at[groups + 2]),
    ]
    later = []
    for i in range(groups):
        start = pl.multiple_of((mine ^ i) * width, width)
        later.append(pltpu.make_async_copy(q_ref.at[:, pl.ds(start, width)], q_out[i], sems.at[i]))
    for copy in first + later:
        copy.start()
    first[0].wait()
    number = lax.broadcasted_iota(jnp.int32, (DOCUMENTS, rows), 0)
    below = jnp.where(seg_buf[...] < number, 1.0, 0.0)
    counts = jnp.broadcast_to(jnp.sum(below, axis=1, keepdims=True), (DOCUMENTS, HEAD_SIZE)).astype(jnp.bfloat16)
    first[1].wait()
    first[2].wait()
    for i in range(groups):
        cut = pl.ds(pl.multiple_of((mine ^ i) * HEAD_SIZE, HEAD_SIZE), HEAD_SIZE)
        kv_out[i][:rows, :] = k_buf[:, cut]
        kv_out[i][rows : 2 * rows, :] = v_buf[:, cut]
        kv_out[i][2 * rows :, :] = counts
    for copy in later:
        copy.wait()


def merge(*refs, groups):
    pieces, near_ref, far_ref = refs[:groups], refs[groups], refs[groups + 1]
    rows = far_ref.shape[1] - DOCUMENTS
    mine = lax.axis_index("group")
    for i in range(groups):
        near_ref[mine ^ i] = pieces[i][...]
        far_ref[mine ^ i, :rows, :] = pieces[i][:rows, :]
        far_ref[mine ^ i, rows:, :] = pieces[i][2 * rows :, :]


def split_values(*refs, groups):
    layers, out = refs[:-groups], refs[-groups:]
    mine = lax.axis_index("group")
    for i in range(groups):
        cut = pl.ds(pl.multiple_of((mine ^ i) * HEAD_SIZE, HEAD_SIZE), HEAD_SIZE)
        for t, ref in enumerate(layers):
            out[i][t] = ref[:, cut]


def join_values(*refs, groups):
    pieces, out_ref = refs[:groups], refs[groups]
    mine = lax.axis_index("group")
    for i in range(groups):
        out_ref[mine ^ i] = pieces[i][...]


def attend(*refs, index, turns, rows, groups, layers, split, final):
    count = len(turns)
    q_ref, home_ref = refs[:2]
    own, mate = refs[2 : 2 + count], refs[2 + count : 2 + 2 * count]
    rest = refs[2 + 2 * count :]
    if final:
        own_values, mate_values = rest[:2]
        state, out_ref, held = rest[2:5], rest[5], rest[6:]
    else:
        held = rest
    m_ref, l_ref, acc_ref, s_ref = held
    per = q_ref.shape[1] // HEAD_SIZE
    chips = own[0].shape[0]
    scale = HEAD_SIZE ** -0.5 * LOG2E
    core, layer = lax.axis_index("core"), lax.axis_index("uly")
    home = lax.axis_index("outer") * groups + (lax.axis_index("group") ^ index)
    shape = (rows, HEAD_SIZE)
    lane = lax.broadcasted_iota(jnp.int32, (DOCUMENTS, HEAD_SIZE), 1).astype(jnp.float32)
    number = lax.broadcasted_iota(jnp.int32, (DOCUMENTS, HEAD_SIZE), 0).astype(jnp.float32)

    def counts(ref, chip):
        return ref[chip, ref.shape[1] - DOCUMENTS :, :].astype(jnp.float32)

    mine = counts(home_ref, home)
    local_row = lax.broadcasted_iota(jnp.int32, shape, 0).astype(jnp.float32)
    row_doc = jnp.zeros(shape, jnp.float32)
    for d in range(DOCUMENTS):
        row_doc = row_doc + jnp.where(jnp.broadcast_to(mine[d : d + 1], shape) <= local_row, 1.0, 0.0)
    place = ((home * 2 + core) * layers + layer) * rows + lax.broadcasted_iota(jnp.int32, shape, 0)
    earliest = row_doc[:1] - 1.0

    def skipped(tiles):
        gone = jnp.zeros((1, HEAD_SIZE), jnp.float32)
        for chip in range(chips):
            least = None
            for ref in tiles:
                held_below = jnp.sum(jnp.where(number == earliest, counts(ref, chip), 0.0), axis=0, keepdims=True)
                least = held_below if least is None else jnp.minimum(least, held_below)
            gone = gone + jnp.where(least >= rows, 1.0, 0.0)
        return jnp.max(gone).astype(jnp.int32)

    m_ref[...] = jnp.full(m_ref.shape, LOW, jnp.float32)
    part = per // split
    heads = list(range(per))
    first_own, first_mate = skipped(own), skipped(mate)
    last_own, last_mate = home + 1, home + core
    second = last_own - first_own

    def strip(h):
        return pl.ds(h * rows, rows)

    def score(tiles, chip, parity, slot):
        k = jnp.concatenate([ref[chip, :rows, :] for ref in tiles], axis=0)
        bias = []
        for turn, ref in zip(turns, tiles):
            base = ((chip * 2 + parity) * layers + (layer ^ turn)) * rows
            key_doc = jnp.sum(jnp.where(counts(ref, chip) <= lane, 1.0, 0.0), axis=0, keepdims=True)
            key = base + lax.broadcasted_iota(jnp.int32, shape, 1)
            bias.append(jnp.where((key <= place) & (row_doc == key_doc), 0.0, LOW))
        for h0 in range(0, per, part):
            q = jnp.concatenate([q_ref[:, h * HEAD_SIZE : (h + 1) * HEAD_SIZE] for h in heads[h0 : h0 + part]], axis=0)
            s = lax.dot_general(q, k, (((1,), (1,)), ((), ())), preferred_element_type=jnp.float32)
            for i in range(part):
                xs = [s[i * rows : (i + 1) * rows, c * rows : (c + 1) * rows] + bias[c] for c in range(count)]
                for c in range(count):
                    s_ref[slot, strip(h0 + i), c * rows : (c + 1) * rows] = xs[c]
                m_ref[strip(h0 + i), :] = functools.reduce(jnp.maximum, xs, m_ref[strip(h0 + i), :])

    def weigh(tiles, values, chip, slot):
        if final:
            v = jnp.concatenate([values[chip, t] for t in range(count)], axis=0)
        else:
            v = jnp.concatenate([ref[chip, rows : 2 * rows, :] for ref in tiles], axis=0)
        for h0 in range(0, per, part):
            ps = []
            for h in heads[h0 : h0 + part]:
                shift = m_ref[strip(h), :]
                p = [
                    jnp.exp2(s_ref[slot, strip(h), c * rows : (c + 1) * rows] * scale - shift) for c in range(count)
                ]
                l_ref[strip(h), :] = functools.reduce(jnp.add, p, l_ref[strip(h), :])
                ps.append(jnp.concatenate([y.astype(jnp.bfloat16) for y in p], axis=1))
            pv = lax.dot_general(
                jnp.concatenate(ps, axis=0), v, (((1,), (0,)), ((), ())), preferred_element_type=jnp.float32
            )
            r = pl.ds(h0 * rows, part * rows)
            acc_ref[r, :] = acc_ref[r, :] + pv

    @pl.loop(first_own, last_own)
    def _(chip):
        score(own, chip, core, chip - first_own)

    @pl.loop(first_mate, last_mate)
    def _(chip):
        score(mate, chip, 1 - core, second + chip - first_mate)

    for h in heads:
        r = strip(h)
        top = jnp.broadcast_to(jnp.max(m_ref[r, :], axis=1, keepdims=True) * scale, shape)
        if final:
            old = state[0][r, :]
            top = jnp.maximum(top, old)
            factor = jnp.exp2(old - top)
            l_ref[r, :] = state[1][r, :] * factor
            acc_ref[r, :] = state[2][r, :] * factor
        else:
            l_ref[r, :] = jnp.zeros(shape, jnp.float32)
            acc_ref[r, :] = jnp.zeros(shape, jnp.float32)
        m_ref[r, :] = top

    @pl.loop(first_own, last_own)
    def _(chip):
        weigh(own, own_values if final else None, chip, chip - first_own)

    @pl.loop(first_mate, last_mate)
    def _(chip):
        weigh(mate, mate_values if final else None, chip, second + chip - first_mate)

    if final:
        for h in heads:
            r = strip(h)
            total = jnp.sum(l_ref[r, :], axis=1, keepdims=True)
            out_ref[:, h * HEAD_SIZE : (h + 1) * HEAD_SIZE] = (acc_ref[r, :] / total).astype(out_ref.dtype)


def place(*refs, groups):
    pieces, out_ref, sems = refs[:groups], refs[groups], refs[groups + 1]
    width = pieces[0].shape[1]
    mine = lax.axis_index("group")
    copies = []
    for i in range(groups):
        start = pl.multiple_of((mine ^ i) * width, width)
        copies.append(pltpu.make_async_copy(pieces[i], out_ref.at[:, pl.ds(start, width)], sems.at[i]))
        copies[-1].start()
    for copy in copies:
        copy.wait()


def limit(mib):
    return pltpu.CompilerParams(vmem_limit_bytes=mib << 20)


def local(queries, keys, values, segments, *, outer, groups, layers):
    rows = queries.shape[0]
    width = queries.shape[1] // groups
    per = width // HEAD_SIZE
    piece = jax.ShapeDtypeStruct((rows, width), jnp.bfloat16)
    one = jax.ShapeDtypeStruct((2 * rows + DOCUMENTS, HEAD_SIZE), jnp.bfloat16)
    made = pl.pallas_call(
        functools.partial(pack, groups=groups),
        out_shape=[one] * groups + [piece] * groups,
        in_specs=[HBM] * 4,
        out_specs=[VMEM] * (2 * groups),
        scratch_shapes=[
            pltpu.VMEM(keys.shape, jnp.bfloat16),
            pltpu.VMEM(values.shape, jnp.bfloat16),
            pltpu.VMEM((1, rows), jnp.int32),
            pltpu.SemaphoreType.DMA((groups + 3,)),
        ],
        compiler_params=limit(8),
        name="pack",
    )(*(pltpu.with_memory_space_constraint(x, pltpu.HBM) for x in (queries, keys, values, segments.reshape(1, rows))))
    kv, q = list(made[:groups]), list(made[groups:])

    def swap(x, axis, size, i):
        return lax.ppermute(x, axis, [(g, g ^ i) for g in range(size)])

    order = list(range(groups - 1, 0, -1))
    near, far = list(range(layers // 2)), list(range(layers // 2, layers))
    for i in order:
        kv[i] = swap(kv[i], "group", groups, i)
    for i in order:
        q[i] = swap(q[i], "group", groups, i)
    block = jax.ShapeDtypeStruct((groups, *one.shape), jnp.bfloat16)
    cut = jax.ShapeDtypeStruct((groups, rows + DOCUMENTS, HEAD_SIZE), jnp.bfloat16)
    mine, keys_only = pl.pallas_call(
        functools.partial(merge, groups=groups),
        out_shape=[block, cut],
        in_specs=[VMEM] * groups,
        out_specs=[VMEM] * 2,
        compiler_params=limit(4),
        name="merge",
    )(*kv)
    raw = [swap(values, "uly", layers, j) for j in far]
    strip = jax.ShapeDtypeStruct((len(far), rows, HEAD_SIZE), jnp.bfloat16)
    v = pl.pallas_call(
        functools.partial(split_values, groups=groups),
        out_shape=[strip] * groups,
        in_specs=[VMEM] * len(far),
        out_specs=[VMEM] * groups,
        compiler_params=limit(4),
        name="split_values",
    )(*raw)
    v = [swap(x, "group", groups, i) if i else x for i, x in enumerate(v)]
    own_values = pl.pallas_call(
        functools.partial(join_values, groups=groups),
        out_shape=jax.ShapeDtypeStruct((groups, *strip.shape), jnp.bfloat16),
        in_specs=[VMEM] * groups,
        out_specs=VMEM,
        compiler_params=limit(4),
        name="join_values",
    )(*v)
    if outer > 1:
        mine, keys_only, own_values = (
            lax.all_gather(x, "outer", axis=0, tiled=True) for x in (mine, keys_only, own_values)
        )
    own = [mine] + [swap(mine if j in near else keys_only, "uly", layers, j) for j in range(1, layers)]

    def across(x):
        return lax.ppermute(x, "core", [(0, 1), (1, 0)])

    mate = [across(own[j]) for j in range(layers)]
    mate_values = across(own_values)

    held = [jax.ShapeDtypeStruct((per * rows, HEAD_SIZE), jnp.float32)] * 3
    common = dict(rows=rows, groups=groups, layers=layers, split=2)
    units = 2 * (outer * groups // 2 + 1)

    def call(i, turns, final, *args):
        return pl.pallas_call(
            functools.partial(attend, index=i, turns=turns, final=final, **common),
            out_shape=piece if final else held,
            in_specs=[VMEM] * len(args),
            out_specs=VMEM if final else [VMEM] * 3,
            scratch_shapes=([pltpu.VMEM(x.shape, x.dtype) for x in held] if final else [])
            + [pltpu.VMEM((units, per * rows, len(turns) * rows), jnp.float32)],
            compiler_params=limit(8 + units),
            name="attend",
        )(*args)

    states = [None] * groups
    last = None
    for i in [0] + order:
        if last is not None:
            q[i], last = lax.optimization_barrier((q[i], last))
        states[i] = call(i, near, False, q[i], own[0], *(own[j] for j in near), *(mate[j] for j in near))
        last = states[i][0]
    out = [None] * groups
    last = None
    for i in order + [0]:
        if last is not None:
            q[i], last = lax.optimization_barrier((q[i], last))
        keyed = [side[j] for side in (own, mate) for j in far]
        last = call(i, far, True, q[i], own[0], *keyed, own_values, mate_values, *states[i])
        out[i] = swap(last, "group", groups, i) if i else last
    return pl.pallas_call(
        functools.partial(place, groups=groups),
        out_shape=jax.ShapeDtypeStruct(queries.shape, jnp.bfloat16),
        in_specs=[VMEM] * groups,
        out_specs=HBM,
        scratch_shapes=[pltpu.SemaphoreType.DMA((groups,))],
        compiler_params=limit(4),
        name="place",
    )(*out)


def solution(mesh):
    blocks, layers = mesh.shape["blk"], mesh.shape["uly"]

    def run(queries, keys, values, segments):
        groups = keys.shape[1] // HEAD_SIZE
        outer = blocks // 2 // groups
        fine = Mesh(mesh.devices.reshape(outer, groups, 2, layers), AXES)

        def body(*args):
            return local(*args, outer=outer, groups=groups, layers=layers)

        spec = P(AXES)
        step = jax.shard_map(body, mesh=fine, in_specs=(spec,) * 4, out_specs=spec, check_vma=False)
        return step(queries, keys, values, segments)

    return run
```

```python
import functools

import jax
import jax.numpy as jnp
from jax import lax
from jax.experimental import pallas as pl
from jax.experimental.pallas import tpu as pltpu
from jax.sharding import Mesh
from jax.sharding import PartitionSpec as P


HEAD_SIZE = 128
DOCUMENTS = 8
LOG2E = 1.4426950408889634
LOW = -1e30
AXES = ("outer", "group", "core", "uly")
VMEM = pl.BlockSpec(memory_space=pltpu.VMEM)
HBM = pl.BlockSpec(memory_space=pltpu.HBM)


def pack(q_ref, k_ref, v_ref, seg_ref, *rest, groups):
    kv_out, q_out, (k_buf, v_buf, seg_buf, sems) = rest[:groups], rest[groups : 2 * groups], rest[2 * groups :]
    rows, width = q_out[0].shape
    mine = lax.axis_index("group")
    first = [
        pltpu.make_async_copy(seg_ref, seg_buf, sems.at[groups]),
        pltpu.make_async_copy(k_ref, k_buf, sems.at[groups + 1]),
        pltpu.make_async_copy(v_ref, v_buf, sems.at[groups + 2]),
    ]
    later = []
    for i in range(groups):
        start = pl.multiple_of((mine ^ i) * width, width)
        later.append(pltpu.make_async_copy(q_ref.at[:, pl.ds(start, width)], q_out[i], sems.at[i]))
    for copy in first + later:
        copy.start()
    first[0].wait()
    number = lax.broadcasted_iota(jnp.int32, (DOCUMENTS, rows), 0)
    below = jnp.where(seg_buf[...] < number, 1.0, 0.0)
    counts = jnp.broadcast_to(jnp.sum(below, axis=1, keepdims=True), (DOCUMENTS, HEAD_SIZE)).astype(jnp.bfloat16)
    first[1].wait()
    first[2].wait()
    for i in range(groups):
        cut = pl.ds(pl.multiple_of((mine ^ i) * HEAD_SIZE, HEAD_SIZE), HEAD_SIZE)
        kv_out[i][:rows, :] = k_buf[:, cut]
        kv_out[i][rows : 2 * rows, :] = v_buf[:, cut]
        kv_out[i][2 * rows :, :] = counts
    for copy in later:
        copy.wait()


def merge(*refs, groups):
    pieces, out_ref = refs[:groups], refs[groups]
    mine = lax.axis_index("group")
    for i in range(groups):
        out_ref[mine ^ i] = pieces[i][...]


def attend(*refs, index, turns, rows, groups, layers, split, final):
    count = len(turns)
    q_ref, home_ref = refs[:2]
    own, mate = refs[2 : 2 + count], refs[2 + count : 2 + 2 * count]
    rest = refs[2 + 2 * count :]
    if final:
        state, out_ref, held = rest[:3], rest[3], rest[4:]
    else:
        held = rest
    m_ref, l_ref, acc_ref, s_ref = held
    per = q_ref.shape[1] // HEAD_SIZE
    chips = own[0].shape[0]
    scale = HEAD_SIZE ** -0.5 * LOG2E
    core, layer = lax.axis_index("core"), lax.axis_index("uly")
    home = lax.axis_index("outer") * groups + (lax.axis_index("group") ^ index)
    shape = (rows, HEAD_SIZE)
    lane = lax.broadcasted_iota(jnp.int32, (DOCUMENTS, HEAD_SIZE), 1).astype(jnp.float32)
    number = lax.broadcasted_iota(jnp.int32, (DOCUMENTS, HEAD_SIZE), 0).astype(jnp.float32)

    def counts(ref, chip):
        return ref[chip, 2 * rows :, :].astype(jnp.float32)

    mine = counts(home_ref, home)
    local_row = lax.broadcasted_iota(jnp.int32, shape, 0).astype(jnp.float32)
    row_doc = jnp.zeros(shape, jnp.float32)
    for d in range(DOCUMENTS):
        row_doc = row_doc + jnp.where(jnp.broadcast_to(mine[d : d + 1], shape) <= local_row, 1.0, 0.0)
    place = ((home * 2 + core) * layers + layer) * rows + lax.broadcasted_iota(jnp.int32, shape, 0)
    earliest = row_doc[:1] - 1.0

    def skipped(tiles):
        gone = jnp.zeros((1, HEAD_SIZE), jnp.float32)
        for chip in range(chips):
            least = None
            for ref in tiles:
                held_below = jnp.sum(jnp.where(number == earliest, counts(ref, chip), 0.0), axis=0, keepdims=True)
                least = held_below if least is None else jnp.minimum(least, held_below)
            gone = gone + jnp.where(least >= rows, 1.0, 0.0)
        return jnp.max(gone).astype(jnp.int32)

    m_ref[...] = jnp.full(m_ref.shape, LOW, jnp.float32)
    part = per // split
    heads = list(range(per))
    first_own, first_mate = skipped(own), skipped(mate)
    last_own, last_mate = home + 1, home + core
    second = last_own - first_own

    def strip(h):
        return pl.ds(h * rows, rows)

    def score(tiles, chip, parity, slot):
        k = jnp.concatenate([ref[chip, :rows, :] for ref in tiles], axis=0)
        bias = []
        for turn, ref in zip(turns, tiles):
            base = ((chip * 2 + parity) * layers + (layer ^ turn)) * rows
            key_doc = jnp.sum(jnp.where(counts(ref, chip) <= lane, 1.0, 0.0), axis=0, keepdims=True)
            key = base + lax.broadcasted_iota(jnp.int32, shape, 1)
            bias.append(jnp.where((key <= place) & (row_doc == key_doc), 0.0, LOW))
        for h0 in range(0, per, part):
            q = jnp.concatenate([q_ref[:, h * HEAD_SIZE : (h + 1) * HEAD_SIZE] for h in heads[h0 : h0 + part]], axis=0)
            s = lax.dot_general(q, k, (((1,), (1,)), ((), ())), preferred_element_type=jnp.float32)
            for i in range(part):
                xs = [s[i * rows : (i + 1) * rows, c * rows : (c + 1) * rows] + bias[c] for c in range(count)]
                for c in range(count):
                    s_ref[slot, strip(h0 + i), c * rows : (c + 1) * rows] = xs[c]
                m_ref[strip(h0 + i), :] = functools.reduce(jnp.maximum, xs, m_ref[strip(h0 + i), :])

    def weigh(tiles, chip, slot):
        v = jnp.concatenate([ref[chip, rows : 2 * rows, :] for ref in tiles], axis=0)
        for h0 in range(0, per, part):
            ps = []
            for h in heads[h0 : h0 + part]:
                shift = m_ref[strip(h), :]
                p = [
                    jnp.exp2(s_ref[slot, strip(h), c * rows : (c + 1) * rows] * scale - shift) for c in range(count)
                ]
                l_ref[strip(h), :] = functools.reduce(jnp.add, p, l_ref[strip(h), :])
                ps.append(jnp.concatenate([y.astype(jnp.bfloat16) for y in p], axis=1))
            pv = lax.dot_general(
                jnp.concatenate(ps, axis=0), v, (((1,), (0,)), ((), ())), preferred_element_type=jnp.float32
            )
            r = pl.ds(h0 * rows, part * rows)
            acc_ref[r, :] = acc_ref[r, :] + pv

    @pl.loop(first_own, last_own)
    def _(chip):
        score(own, chip, core, chip - first_own)

    @pl.loop(first_mate, last_mate)
    def _(chip):
        score(mate, chip, 1 - core, second + chip - first_mate)

    for h in heads:
        r = strip(h)
        top = jnp.broadcast_to(jnp.max(m_ref[r, :], axis=1, keepdims=True) * scale, shape)
        if final:
            old = state[0][r, :]
            top = jnp.maximum(top, old)
            factor = jnp.exp2(old - top)
            l_ref[r, :] = state[1][r, :] * factor
            acc_ref[r, :] = state[2][r, :] * factor
        else:
            l_ref[r, :] = jnp.zeros(shape, jnp.float32)
            acc_ref[r, :] = jnp.zeros(shape, jnp.float32)
        m_ref[r, :] = top

    @pl.loop(first_own, last_own)
    def _(chip):
        weigh(own, chip, chip - first_own)

    @pl.loop(first_mate, last_mate)
    def _(chip):
        weigh(mate, chip, second + chip - first_mate)

    if final:
        for h in heads:
            r = strip(h)
            total = jnp.sum(l_ref[r, :], axis=1, keepdims=True)
            out_ref[:, h * HEAD_SIZE : (h + 1) * HEAD_SIZE] = (acc_ref[r, :] / total).astype(out_ref.dtype)


def place(*refs, groups):
    pieces, out_ref, sems = refs[:groups], refs[groups], refs[groups + 1]
    width = pieces[0].shape[1]
    mine = lax.axis_index("group")
    copies = []
    for i in range(groups):
        start = pl.multiple_of((mine ^ i) * width, width)
        copies.append(pltpu.make_async_copy(pieces[i], out_ref.at[:, pl.ds(start, width)], sems.at[i]))
        copies[-1].start()
    for copy in copies:
        copy.wait()


def limit(mib):
    return pltpu.CompilerParams(vmem_limit_bytes=mib << 20)


def local(queries, keys, values, segments, *, outer, groups, layers):
    rows = queries.shape[0]
    width = queries.shape[1] // groups
    per = width // HEAD_SIZE
    piece = jax.ShapeDtypeStruct((rows, width), jnp.bfloat16)
    one = jax.ShapeDtypeStruct((2 * rows + DOCUMENTS, HEAD_SIZE), jnp.bfloat16)
    made = pl.pallas_call(
        functools.partial(pack, groups=groups),
        out_shape=[one] * groups + [piece] * groups,
        in_specs=[HBM] * 4,
        out_specs=[VMEM] * (2 * groups),
        scratch_shapes=[
            pltpu.VMEM(keys.shape, jnp.bfloat16),
            pltpu.VMEM(values.shape, jnp.bfloat16),
            pltpu.VMEM((1, rows), jnp.int32),
            pltpu.SemaphoreType.DMA((groups + 3,)),
        ],
        compiler_params=limit(8),
        name="pack",
    )(*(pltpu.with_memory_space_constraint(x, pltpu.HBM) for x in (queries, keys, values, segments.reshape(1, rows))))
    kv, q = list(made[:groups]), list(made[groups:])

    def swap(x, axis, size, i):
        return lax.ppermute(x, axis, [(g, g ^ i) for g in range(size)])

    order = list(range(groups - 1, 0, -1))
    for i in order:
        kv[i] = swap(kv[i], "group", groups, i)
    for i in order:
        q[i] = swap(q[i], "group", groups, i)
    mine = pl.pallas_call(
        functools.partial(merge, groups=groups),
        out_shape=jax.ShapeDtypeStruct((groups, *one.shape), jnp.bfloat16),
        in_specs=[VMEM] * groups,
        out_specs=VMEM,
        compiler_params=limit(4),
        name="merge",
    )(*kv)
    if outer > 1:
        mine = lax.all_gather(mine, "outer", axis=0, tiled=True)
    own = [mine] + [swap(mine, "uly", layers, j) for j in range(1, layers)]
    mate = []
    for j in range(layers):
        mate.append(lax.ppermute(own[j], "core", [(0, 1), (1, 0)]))

    held = [jax.ShapeDtypeStruct((per * rows, HEAD_SIZE), jnp.float32)] * 3
    common = dict(rows=rows, groups=groups, layers=layers, split=2)
    units = 2 * (outer * groups // 2 + 1)
    near, far = list(range(layers // 2)), list(range(layers // 2, layers))

    def call(i, turns, final, *args):
        return pl.pallas_call(
            functools.partial(attend, index=i, turns=turns, final=final, **common),
            out_shape=piece if final else held,
            in_specs=[VMEM] * len(args),
            out_specs=VMEM if final else [VMEM] * 3,
            scratch_shapes=([pltpu.VMEM(x.shape, x.dtype) for x in held] if final else [])
            + [pltpu.VMEM((units, per * rows, len(turns) * rows), jnp.float32)],
            compiler_params=limit(8 + units),
            name="attend",
        )(*args)

    states = [None] * groups
    last = None
    for i in [0] + order:
        if last is not None:
            q[i], last = lax.optimization_barrier((q[i], last))
        states[i] = call(i, near, False, q[i], own[0], *(own[j] for j in near), *(mate[j] for j in near))
        last = states[i][0]
    out = [None] * groups
    last = None
    for i in order + [0]:
        if last is not None:
            q[i], last = lax.optimization_barrier((q[i], last))
        last = call(i, far, True, q[i], own[0], *(own[j] for j in far), *(mate[j] for j in far), *states[i])
        out[i] = swap(last, "group", groups, i) if i else last
    return pl.pallas_call(
        functools.partial(place, groups=groups),
        out_shape=jax.ShapeDtypeStruct(queries.shape, jnp.bfloat16),
        in_specs=[VMEM] * groups,
        out_specs=HBM,
        scratch_shapes=[pltpu.SemaphoreType.DMA((groups,))],
        compiler_params=limit(4),
        name="place",
    )(*out)


def solution(mesh):
    blocks, layers = mesh.shape["blk"], mesh.shape["uly"]

    def run(queries, keys, values, segments):
        groups = keys.shape[1] // HEAD_SIZE
        outer = blocks // 2 // groups
        fine = Mesh(mesh.devices.reshape(outer, groups, 2, layers), AXES)

        def body(*args):
            return local(*args, outer=outer, groups=groups, layers=layers)

        spec = P(AXES)
        step = jax.shard_map(body, mesh=fine, in_specs=(spec,) * 4, out_specs=spec, check_vma=False)
        return step(queries, keys, values, segments)

    return run
```

```python
import functools

import jax
import jax.numpy as jnp
from jax import lax
from jax.experimental import pallas as pl
from jax.experimental.pallas import tpu as pltpu
from jax.sharding import Mesh
from jax.sharding import PartitionSpec as P


HEAD_SIZE = 128
DOCUMENTS = 8
LOG2E = 1.4426950408889634
LOW = -1e30
AXES = ("outer", "group", "core", "uly")
VMEM = pl.BlockSpec(memory_space=pltpu.VMEM)
HBM = pl.BlockSpec(memory_space=pltpu.HBM)


def pack(k_ref, v_ref, seg_ref, *rest, groups):
    out, (k_buf, v_buf, seg_buf, sems) = rest[:groups], rest[groups:]
    rows = k_buf.shape[0]
    mine = lax.axis_index("group")
    pairs = ((seg_ref, seg_buf), (k_ref, k_buf), (v_ref, v_buf))
    copies = [pltpu.make_async_copy(x, y, sems.at[i]) for i, (x, y) in enumerate(pairs)]
    for copy in copies:
        copy.start()
    copies[0].wait()
    number = lax.broadcasted_iota(jnp.int32, (DOCUMENTS, rows), 0)
    below = jnp.where(seg_buf[...] < number, 1.0, 0.0)
    counts = jnp.broadcast_to(jnp.sum(below, axis=1, keepdims=True), (DOCUMENTS, HEAD_SIZE)).astype(jnp.bfloat16)
    copies[1].wait()
    copies[2].wait()
    for i in range(groups):
        cut = pl.ds(pl.multiple_of((mine ^ i) * HEAD_SIZE, HEAD_SIZE), HEAD_SIZE)
        out[i][:rows, :] = k_buf[:, cut]
        out[i][rows : 2 * rows, :] = v_buf[:, cut]
        out[i][2 * rows :, :] = counts


def pack_queries(q_ref, *rest, groups):
    out, sems = rest[:groups], rest[groups]
    width = out[0].shape[1]
    mine = lax.axis_index("group")
    copies = []
    for i in range(groups):
        start = pl.multiple_of((mine ^ i) * width, width)
        copies.append(pltpu.make_async_copy(q_ref.at[:, pl.ds(start, width)], out[i], sems.at[i]))
        copies[-1].start()
    for copy in copies:
        copy.wait()


def merge(*refs, groups):
    pieces, out_ref = refs[:groups], refs[groups]
    mine = lax.axis_index("group")
    for i in range(groups):
        out_ref[mine ^ i] = pieces[i][...]


def attend(*refs, index, turns, rows, groups, layers, split, final):
    count = len(turns)
    q_ref, home_ref = refs[:2]
    own, mate = refs[2 : 2 + count], refs[2 + count : 2 + 2 * count]
    rest = refs[2 + 2 * count :]
    if final:
        state, out_ref, held = rest[:3], rest[3], rest[4:]
    else:
        held = rest
    m_ref, l_ref, acc_ref, s_ref = held
    per = q_ref.shape[1] // HEAD_SIZE
    chips = own[0].shape[0]
    scale = HEAD_SIZE ** -0.5 * LOG2E
    core, layer = lax.axis_index("core"), lax.axis_index("uly")
    home = lax.axis_index("outer") * groups + (lax.axis_index("group") ^ index)
    shape = (rows, HEAD_SIZE)
    lane = lax.broadcasted_iota(jnp.int32, (DOCUMENTS, HEAD_SIZE), 1).astype(jnp.float32)
    number = lax.broadcasted_iota(jnp.int32, (DOCUMENTS, HEAD_SIZE), 0).astype(jnp.float32)

    def counts(ref, chip):
        return ref[chip, 2 * rows :, :].astype(jnp.float32)

    mine = counts(home_ref, home)
    local_row = lax.broadcasted_iota(jnp.int32, shape, 0).astype(jnp.float32)
    row_doc = jnp.zeros(shape, jnp.float32)
    for d in range(DOCUMENTS):
        row_doc = row_doc + jnp.where(jnp.broadcast_to(mine[d : d + 1], shape) <= local_row, 1.0, 0.0)
    place = ((home * 2 + core) * layers + layer) * rows + lax.broadcasted_iota(jnp.int32, shape, 0)
    earliest = row_doc[:1] - 1.0

    def skipped(tiles):
        gone = jnp.zeros((1, HEAD_SIZE), jnp.float32)
        for chip in range(chips):
            least = None
            for ref in tiles:
                held_below = jnp.sum(jnp.where(number == earliest, counts(ref, chip), 0.0), axis=0, keepdims=True)
                least = held_below if least is None else jnp.minimum(least, held_below)
            gone = gone + jnp.where(least >= rows, 1.0, 0.0)
        return jnp.max(gone).astype(jnp.int32)

    m_ref[...] = jnp.full(m_ref.shape, LOW, jnp.float32)
    part = per // split
    heads = list(range(per))
    first_own, first_mate = skipped(own), skipped(mate)
    last_own, last_mate = home + 1, home + core
    second = last_own - first_own

    def strip(h):
        return pl.ds(h * rows, rows)

    def score(tiles, chip, parity, slot):
        k = jnp.concatenate([ref[chip, :rows, :] for ref in tiles], axis=0)
        bias = []
        for turn, ref in zip(turns, tiles):
            base = ((chip * 2 + parity) * layers + (layer ^ turn)) * rows
            key_doc = jnp.sum(jnp.where(counts(ref, chip) <= lane, 1.0, 0.0), axis=0, keepdims=True)
            key = base + lax.broadcasted_iota(jnp.int32, shape, 1)
            bias.append(jnp.where((key <= place) & (row_doc == key_doc), 0.0, LOW))
        for h0 in range(0, per, part):
            q = jnp.concatenate([q_ref[:, h * HEAD_SIZE : (h + 1) * HEAD_SIZE] for h in heads[h0 : h0 + part]], axis=0)
            s = lax.dot_general(q, k, (((1,), (1,)), ((), ())), preferred_element_type=jnp.float32)
            for i in range(part):
                xs = [s[i * rows : (i + 1) * rows, c * rows : (c + 1) * rows] + bias[c] for c in range(count)]
                for c in range(count):
                    s_ref[slot, strip(h0 + i), c * rows : (c + 1) * rows] = xs[c]
                m_ref[strip(h0 + i), :] = functools.reduce(jnp.maximum, xs, m_ref[strip(h0 + i), :])

    def weigh(tiles, chip, slot):
        v = jnp.concatenate([ref[chip, rows : 2 * rows, :] for ref in tiles], axis=0)
        for h0 in range(0, per, part):
            ps = []
            for h in heads[h0 : h0 + part]:
                shift = m_ref[strip(h), :]
                p = [
                    jnp.exp2(s_ref[slot, strip(h), c * rows : (c + 1) * rows] * scale - shift) for c in range(count)
                ]
                l_ref[strip(h), :] = functools.reduce(jnp.add, p, l_ref[strip(h), :])
                ps.append(jnp.concatenate([y.astype(jnp.bfloat16) for y in p], axis=1))
            pv = lax.dot_general(
                jnp.concatenate(ps, axis=0), v, (((1,), (0,)), ((), ())), preferred_element_type=jnp.float32
            )
            r = pl.ds(h0 * rows, part * rows)
            acc_ref[r, :] = acc_ref[r, :] + pv

    @pl.loop(first_own, last_own)
    def _(chip):
        score(own, chip, core, chip - first_own)

    @pl.loop(first_mate, last_mate)
    def _(chip):
        score(mate, chip, 1 - core, second + chip - first_mate)

    for h in heads:
        r = strip(h)
        top = jnp.broadcast_to(jnp.max(m_ref[r, :], axis=1, keepdims=True) * scale, shape)
        if final:
            old = state[0][r, :]
            top = jnp.maximum(top, old)
            factor = jnp.exp2(old - top)
            l_ref[r, :] = state[1][r, :] * factor
            acc_ref[r, :] = state[2][r, :] * factor
        else:
            l_ref[r, :] = jnp.zeros(shape, jnp.float32)
            acc_ref[r, :] = jnp.zeros(shape, jnp.float32)
        m_ref[r, :] = top

    @pl.loop(first_own, last_own)
    def _(chip):
        weigh(own, chip, chip - first_own)

    @pl.loop(first_mate, last_mate)
    def _(chip):
        weigh(mate, chip, second + chip - first_mate)

    if final:
        for h in heads:
            r = strip(h)
            total = jnp.sum(l_ref[r, :], axis=1, keepdims=True)
            out_ref[:, h * HEAD_SIZE : (h + 1) * HEAD_SIZE] = (acc_ref[r, :] / total).astype(out_ref.dtype)


def place(*refs, groups):
    pieces, out_ref, sems = refs[:groups], refs[groups], refs[groups + 1]
    width = pieces[0].shape[1]
    mine = lax.axis_index("group")
    copies = []
    for i in range(groups):
        start = pl.multiple_of((mine ^ i) * width, width)
        copies.append(pltpu.make_async_copy(pieces[i], out_ref.at[:, pl.ds(start, width)], sems.at[i]))
        copies[-1].start()
    for copy in copies:
        copy.wait()


def limit(mib):
    return pltpu.CompilerParams(vmem_limit_bytes=mib << 20)


def local(queries, keys, values, segments, *, outer, groups, layers):
    rows = queries.shape[0]
    width = queries.shape[1] // groups
    per = width // HEAD_SIZE
    piece = jax.ShapeDtypeStruct((rows, width), jnp.bfloat16)
    one = jax.ShapeDtypeStruct((2 * rows + DOCUMENTS, HEAD_SIZE), jnp.bfloat16)
    raw = [pltpu.with_memory_space_constraint(x, pltpu.HBM) for x in (keys, values, segments.reshape(1, rows), queries)]
    kv = list(
        pl.pallas_call(
            functools.partial(pack, groups=groups),
            out_shape=[one] * groups,
            in_specs=[HBM] * 3,
            out_specs=[VMEM] * groups,
            scratch_shapes=[
                pltpu.VMEM(keys.shape, jnp.bfloat16),
                pltpu.VMEM(values.shape, jnp.bfloat16),
                pltpu.VMEM((1, rows), jnp.int32),
                pltpu.SemaphoreType.DMA((3,)),
            ],
            compiler_params=limit(4),
            name="pack",
        )(*raw[:3])
    )
    q = list(
        pl.pallas_call(
            functools.partial(pack_queries, groups=groups),
            out_shape=[piece] * groups,
            in_specs=[HBM],
            out_specs=[VMEM] * groups,
            scratch_shapes=[pltpu.SemaphoreType.DMA((groups,))],
            compiler_params=limit(4),
            name="pack_queries",
        )(raw[3])
    )

    def swap(x, axis, size, i):
        return lax.ppermute(x, axis, [(g, g ^ i) for g in range(size)])

    order = list(range(groups - 1, 0, -1))
    for i in order:
        kv[i] = swap(kv[i], "group", groups, i)
    for i in order:
        q[i] = swap(q[i], "group", groups, i)
    mine = pl.pallas_call(
        functools.partial(merge, groups=groups),
        out_shape=jax.ShapeDtypeStruct((groups, *one.shape), jnp.bfloat16),
        in_specs=[VMEM] * groups,
        out_specs=VMEM,
        compiler_params=limit(4),
        name="merge",
    )(*kv)
    if outer > 1:
        mine = lax.all_gather(mine, "outer", axis=0, tiled=True)
    own = [mine] + [swap(mine, "uly", layers, j) for j in range(1, layers)]
    mate = []
    for j in range(layers):
        mate.append(lax.ppermute(own[j], "core", [(0, 1), (1, 0)]))

    held = [jax.ShapeDtypeStruct((per * rows, HEAD_SIZE), jnp.float32)] * 3
    common = dict(rows=rows, groups=groups, layers=layers, split=2)
    units = 2 * (outer * groups // 2 + 1)
    near, far = list(range(layers // 2)), list(range(layers // 2, layers))

    def call(i, turns, final, *args):
        return pl.pallas_call(
            functools.partial(attend, index=i, turns=turns, final=final, **common),
            out_shape=piece if final else held,
            in_specs=[VMEM] * len(args),
            out_specs=VMEM if final else [VMEM] * 3,
            scratch_shapes=([pltpu.VMEM(x.shape, x.dtype) for x in held] if final else [])
            + [pltpu.VMEM((units, per * rows, len(turns) * rows), jnp.float32)],
            compiler_params=limit(8 + units),
            name="attend",
        )(*args)

    states = [None] * groups
    last = None
    for i in [0] + order:
        if last is not None:
            q[i], last = lax.optimization_barrier((q[i], last))
        states[i] = call(i, near, False, q[i], own[0], *(own[j] for j in near), *(mate[j] for j in near))
        last = states[i][0]
    out = [None] * groups
    last = None
    for i in order + [0]:
        if last is not None:
            q[i], last = lax.optimization_barrier((q[i], last))
        last = call(i, far, True, q[i], own[0], *(own[j] for j in far), *(mate[j] for j in far), *states[i])
        out[i] = swap(last, "group", groups, i) if i else last
    return pl.pallas_call(
        functools.partial(place, groups=groups),
        out_shape=jax.ShapeDtypeStruct(queries.shape, jnp.bfloat16),
        in_specs=[VMEM] * groups,
        out_specs=HBM,
        scratch_shapes=[pltpu.SemaphoreType.DMA((groups,))],
        compiler_params=limit(4),
        name="place",
    )(*out)


def solution(mesh):
    blocks, layers = mesh.shape["blk"], mesh.shape["uly"]

    def run(queries, keys, values, segments):
        groups = keys.shape[1] // HEAD_SIZE
        outer = blocks // 2 // groups
        fine = Mesh(mesh.devices.reshape(outer, groups, 2, layers), AXES)

        def body(*args):
            return local(*args, outer=outer, groups=groups, layers=layers)

        spec = P(AXES)
        step = jax.shard_map(body, mesh=fine, in_specs=(spec,) * 4, out_specs=spec, check_vma=False)
        return step(queries, keys, values, segments)

    return run
```

```python
import functools

import jax
import jax.numpy as jnp
from jax import lax
from jax.experimental import pallas as pl
from jax.experimental.pallas import tpu as pltpu
from jax.sharding import Mesh
from jax.sharding import PartitionSpec as P


HEAD_SIZE = 128
DOCUMENTS = 8
LOG2E = 1.4426950408889634
LOW = -1e30
AXES = ("outer", "group", "core", "uly")
VMEM = pl.BlockSpec(memory_space=pltpu.VMEM)
HBM = pl.BlockSpec(memory_space=pltpu.HBM)


def pack(k_ref, v_ref, seg_ref, *rest, groups):
    out, (k_buf, v_buf, seg_buf, sems) = rest[:groups], rest[groups:]
    rows = k_buf.shape[0]
    mine = lax.axis_index("group")
    pairs = ((seg_ref, seg_buf), (k_ref, k_buf), (v_ref, v_buf))
    copies = [pltpu.make_async_copy(x, y, sems.at[i]) for i, (x, y) in enumerate(pairs)]
    for copy in copies:
        copy.start()
    copies[0].wait()
    number = lax.broadcasted_iota(jnp.int32, (DOCUMENTS, rows), 0)
    below = jnp.where(seg_buf[...] < number, 1.0, 0.0)
    counts = jnp.broadcast_to(jnp.sum(below, axis=1, keepdims=True), (DOCUMENTS, HEAD_SIZE)).astype(jnp.bfloat16)
    copies[1].wait()
    copies[2].wait()
    for i in range(groups):
        cut = pl.ds(pl.multiple_of((mine ^ i) * HEAD_SIZE, HEAD_SIZE), HEAD_SIZE)
        out[i][:rows, :] = k_buf[:, cut]
        out[i][rows : 2 * rows, :] = v_buf[:, cut]
        out[i][2 * rows :, :] = counts


def pack_queries(q_ref, *rest, groups):
    out, sems = rest[:groups], rest[groups]
    width = out[0].shape[1]
    mine = lax.axis_index("group")
    copies = []
    for i in range(groups):
        start = pl.multiple_of((mine ^ i) * width, width)
        copies.append(pltpu.make_async_copy(q_ref.at[:, pl.ds(start, width)], out[i], sems.at[i]))
        copies[-1].start()
    for copy in copies:
        copy.wait()


def merge(*refs, groups):
    pieces, out_ref = refs[:groups], refs[groups]
    mine = lax.axis_index("group")
    for i in range(groups):
        out_ref[mine ^ i] = pieces[i][...]


def attend(*refs, index, turns, rows, groups, layers, split, sides, resume, final):
    count = len(turns)
    q_ref, home_ref = refs[:2]
    refs = refs[2:]
    tiles = []
    for side in sides:
        tiles.append(refs[:count] if side else ())
        refs = refs[len(tiles[-1]) :]
    own, mate = tiles
    state, refs = (refs[:3], refs[3:]) if resume else (None, refs)
    out_ref, held = (refs[0], refs[1:]) if final else (None, refs)
    m_ref, l_ref, acc_ref, s_ref = held
    per = q_ref.shape[1] // HEAD_SIZE
    chips = home_ref.shape[0]
    scale = HEAD_SIZE ** -0.5 * LOG2E
    core, layer = lax.axis_index("core"), lax.axis_index("uly")
    home = lax.axis_index("outer") * groups + (lax.axis_index("group") ^ index)
    shape = (rows, HEAD_SIZE)
    lane = lax.broadcasted_iota(jnp.int32, (DOCUMENTS, HEAD_SIZE), 1).astype(jnp.float32)
    number = lax.broadcasted_iota(jnp.int32, (DOCUMENTS, HEAD_SIZE), 0).astype(jnp.float32)

    def counts(ref, chip):
        return ref[chip, 2 * rows :, :].astype(jnp.float32)

    mine = counts(home_ref, home)
    local_row = lax.broadcasted_iota(jnp.int32, shape, 0).astype(jnp.float32)
    row_doc = jnp.zeros(shape, jnp.float32)
    for d in range(DOCUMENTS):
        row_doc = row_doc + jnp.where(jnp.broadcast_to(mine[d : d + 1], shape) <= local_row, 1.0, 0.0)
    place = ((home * 2 + core) * layers + layer) * rows + lax.broadcasted_iota(jnp.int32, shape, 0)
    earliest = row_doc[:1] - 1.0

    def skipped(tiles):
        gone = jnp.zeros((1, HEAD_SIZE), jnp.float32)
        for chip in range(chips):
            least = None
            for ref in tiles:
                held_below = jnp.sum(jnp.where(number == earliest, counts(ref, chip), 0.0), axis=0, keepdims=True)
                least = held_below if least is None else jnp.minimum(least, held_below)
            gone = gone + jnp.where(least >= rows, 1.0, 0.0)
        return jnp.max(gone).astype(jnp.int32)

    m_ref[...] = jnp.full(m_ref.shape, LOW, jnp.float32)
    part = per // split
    heads = list(range(per))
    last_own, last_mate = home + 1, home + core
    first_own = skipped(own) if own else last_own
    first_mate = skipped(mate) if mate else last_mate
    second = last_own - first_own

    def strip(h):
        return pl.ds(h * rows, rows)

    def score(tiles, chip, parity, slot):
        k = jnp.concatenate([ref[chip, :rows, :] for ref in tiles], axis=0)
        bias = []
        for turn, ref in zip(turns, tiles):
            base = ((chip * 2 + parity) * layers + (layer ^ turn)) * rows
            key_doc = jnp.sum(jnp.where(counts(ref, chip) <= lane, 1.0, 0.0), axis=0, keepdims=True)
            key = base + lax.broadcasted_iota(jnp.int32, shape, 1)
            bias.append(jnp.where((key <= place) & (row_doc == key_doc), 0.0, LOW))
        for h0 in range(0, per, part):
            q = jnp.concatenate([q_ref[:, h * HEAD_SIZE : (h + 1) * HEAD_SIZE] for h in heads[h0 : h0 + part]], axis=0)
            s = lax.dot_general(q, k, (((1,), (1,)), ((), ())), preferred_element_type=jnp.float32)
            for i in range(part):
                xs = [s[i * rows : (i + 1) * rows, c * rows : (c + 1) * rows] + bias[c] for c in range(count)]
                for c in range(count):
                    s_ref[slot, strip(h0 + i), c * rows : (c + 1) * rows] = xs[c]
                m_ref[strip(h0 + i), :] = functools.reduce(jnp.maximum, xs, m_ref[strip(h0 + i), :])

    def weigh(tiles, chip, slot):
        v = jnp.concatenate([ref[chip, rows : 2 * rows, :] for ref in tiles], axis=0)
        for h0 in range(0, per, part):
            ps = []
            for h in heads[h0 : h0 + part]:
                shift = m_ref[strip(h), :]
                p = [
                    jnp.exp2(s_ref[slot, strip(h), c * rows : (c + 1) * rows] * scale - shift) for c in range(count)
                ]
                l_ref[strip(h), :] = functools.reduce(jnp.add, p, l_ref[strip(h), :])
                ps.append(jnp.concatenate([y.astype(jnp.bfloat16) for y in p], axis=1))
            pv = lax.dot_general(
                jnp.concatenate(ps, axis=0), v, (((1,), (0,)), ((), ())), preferred_element_type=jnp.float32
            )
            r = pl.ds(h0 * rows, part * rows)
            acc_ref[r, :] = acc_ref[r, :] + pv

    if own:

        @pl.loop(first_own, last_own)
        def _(chip):
            score(own, chip, core, chip - first_own)

    if mate:

        @pl.loop(first_mate, last_mate)
        def _(chip):
            score(mate, chip, 1 - core, second + chip - first_mate)

    for h in heads:
        r = strip(h)
        top = jnp.broadcast_to(jnp.max(m_ref[r, :], axis=1, keepdims=True) * scale, shape)
        if resume:
            old = state[0][r, :]
            top = jnp.maximum(top, old)
            factor = jnp.exp2(old - top)
            l_ref[r, :] = state[1][r, :] * factor
            acc_ref[r, :] = state[2][r, :] * factor
        else:
            l_ref[r, :] = jnp.zeros(shape, jnp.float32)
            acc_ref[r, :] = jnp.zeros(shape, jnp.float32)
        m_ref[r, :] = top

    if own:

        @pl.loop(first_own, last_own)
        def _(chip):
            weigh(own, chip, chip - first_own)

    if mate:

        @pl.loop(first_mate, last_mate)
        def _(chip):
            weigh(mate, chip, second + chip - first_mate)

    if final:
        for h in heads:
            r = strip(h)
            total = jnp.sum(l_ref[r, :], axis=1, keepdims=True)
            out_ref[:, h * HEAD_SIZE : (h + 1) * HEAD_SIZE] = (acc_ref[r, :] / total).astype(out_ref.dtype)


def place(*refs, turns):
    pieces, out_ref, sems = refs[: len(turns)], refs[-2], refs[-1]
    width = pieces[0].shape[1]
    mine = lax.axis_index("group")
    copies = []
    for i, piece in zip(turns, pieces):
        start = pl.multiple_of((mine ^ i) * width, width)
        copies.append(pltpu.make_async_copy(piece, out_ref.at[:, pl.ds(start, width)], sems.at[i]))
        copies[-1].start()
    for copy in copies:
        copy.wait()


def limit(mib):
    return pltpu.CompilerParams(vmem_limit_bytes=mib << 20)


def local(queries, keys, values, segments, *, outer, groups, layers):
    rows = queries.shape[0]
    width = queries.shape[1] // groups
    per = width // HEAD_SIZE
    piece = jax.ShapeDtypeStruct((rows, width), jnp.bfloat16)
    one = jax.ShapeDtypeStruct((2 * rows + DOCUMENTS, HEAD_SIZE), jnp.bfloat16)
    raw = [pltpu.with_memory_space_constraint(x, pltpu.HBM) for x in (keys, values, segments.reshape(1, rows), queries)]
    kv = list(
        pl.pallas_call(
            functools.partial(pack, groups=groups),
            out_shape=[one] * groups,
            in_specs=[HBM] * 3,
            out_specs=[VMEM] * groups,
            scratch_shapes=[
                pltpu.VMEM(keys.shape, jnp.bfloat16),
                pltpu.VMEM(values.shape, jnp.bfloat16),
                pltpu.VMEM((1, rows), jnp.int32),
                pltpu.SemaphoreType.DMA((3,)),
            ],
            compiler_params=limit(4),
            name="pack",
        )(*raw[:3])
    )
    q = list(
        pl.pallas_call(
            functools.partial(pack_queries, groups=groups),
            out_shape=[piece] * groups,
            in_specs=[HBM],
            out_specs=[VMEM] * groups,
            scratch_shapes=[pltpu.SemaphoreType.DMA((groups,))],
            compiler_params=limit(4),
            name="pack_queries",
        )(raw[3])
    )

    def swap(x, axis, size, i):
        return lax.ppermute(x, axis, [(g, g ^ i) for g in range(size)])

    order = list(range(groups - 1, 0, -1))
    for i in order:
        kv[i] = swap(kv[i], "group", groups, i)
    for i in order:
        q[i] = swap(q[i], "group", groups, i)
    mine = pl.pallas_call(
        functools.partial(merge, groups=groups),
        out_shape=jax.ShapeDtypeStruct((groups, *one.shape), jnp.bfloat16),
        in_specs=[VMEM] * groups,
        out_specs=VMEM,
        compiler_params=limit(4),
        name="merge",
    )(*kv)
    if outer > 1:
        mine = lax.all_gather(mine, "outer", axis=0, tiled=True)
    own = [mine] + [swap(mine, "uly", layers, j) for j in range(1, layers)]
    mate = []
    for j in range(layers):
        mate.append(lax.ppermute(own[j], "core", [(0, 1), (1, 0)]))

    held = [jax.ShapeDtypeStruct((per * rows, HEAD_SIZE), jnp.float32)] * 3
    common = dict(rows=rows, groups=groups, layers=layers, split=2)
    units = 2 * (outer * groups // 2 + 1)
    near, far = list(range(layers // 2)), list(range(layers // 2, layers))

    def call(i, turns, sides, state, final):
        args = [q[i], own[0]]
        for side, held_by in zip(sides, (own, mate)):
            args += [held_by[j] for j in turns] if side else []
        args += state or []
        keep = dict(sides=sides, resume=state is not None, final=final)
        return pl.pallas_call(
            functools.partial(attend, index=i, turns=turns, **keep, **common),
            out_shape=piece if final else held,
            in_specs=[VMEM] * len(args),
            out_specs=VMEM if final else [VMEM] * 3,
            scratch_shapes=([pltpu.VMEM(x.shape, x.dtype) for x in held] if final else [])
            + [pltpu.VMEM((units, per * rows, len(turns) * rows), jnp.float32)],
            compiler_params=limit(8 + units),
            name="attend",
        )(*args)

    both, states, out, last = (True, True), [None] * groups, [None] * groups, None

    def follow(i):
        nonlocal last
        if last is not None:
            q[i], last = lax.optimization_barrier((q[i], last))

    for i in [0] + order:
        follow(i)
        states[i] = call(i, near, both, None, False)
        last = states[i][0]
    i = order[0]
    follow(i)
    states[i] = call(i, far, (True, False), states[i], False)
    last = states[i][0]
    for i in order + [0]:
        follow(i)
        last = call(i, far, (False, True) if i == order[0] else both, states[i], True)
        out[i] = swap(last, "group", groups, i) if i else last

    def put(turns, *rest):
        return pl.pallas_call(
            functools.partial(place, turns=turns),
            out_shape=jax.ShapeDtypeStruct(queries.shape, jnp.bfloat16),
            in_specs=[VMEM] * len(turns) + [HBM] * len(rest),
            out_specs=HBM,
            scratch_shapes=[pltpu.SemaphoreType.DMA((groups,))],
            input_output_aliases={len(turns): 0} if rest else {},
            compiler_params=limit(4),
            name="place",
        )(*(out[i] for i in turns), *rest)

    return put(order[-1:], put([0] + order[:-1]))


def solution(mesh):
    blocks, layers = mesh.shape["blk"], mesh.shape["uly"]

    def run(queries, keys, values, segments):
        groups = keys.shape[1] // HEAD_SIZE
        outer = blocks // 2 // groups
        fine = Mesh(mesh.devices.reshape(outer, groups, 2, layers), AXES)

        def body(*args):
            return local(*args, outer=outer, groups=groups, layers=layers)

        spec = P(AXES)
        step = jax.shard_map(body, mesh=fine, in_specs=(spec,) * 4, out_specs=spec, check_vma=False)
        return step(queries, keys, values, segments)

    return run
```

```python
import functools

import jax
import jax.numpy as jnp
from jax import lax
from jax.experimental import pallas as pl
from jax.experimental.pallas import tpu as pltpu
from jax.sharding import Mesh
from jax.sharding import PartitionSpec as P


HEAD_SIZE = 128
DOCUMENTS = 8
LOG2E = 1.4426950408889634
LOW = -1e30
AXES = ("outer", "group", "core", "uly")
VMEM = pl.BlockSpec(memory_space=pltpu.VMEM)
HBM = pl.BlockSpec(memory_space=pltpu.HBM)


def pack(k_ref, v_ref, seg_ref, *rest, groups):
    out, (k_buf, v_buf, seg_buf, sems) = rest[:groups], rest[groups:]
    rows = k_buf.shape[0]
    mine = lax.axis_index("group")
    pairs = ((seg_ref, seg_buf), (k_ref, k_buf), (v_ref, v_buf))
    copies = [pltpu.make_async_copy(x, y, sems.at[i]) for i, (x, y) in enumerate(pairs)]
    for copy in copies:
        copy.start()
    copies[0].wait()
    number = lax.broadcasted_iota(jnp.int32, (DOCUMENTS, rows), 0)
    below = jnp.where(seg_buf[...] < number, 1.0, 0.0)
    counts = jnp.broadcast_to(jnp.sum(below, axis=1, keepdims=True), (DOCUMENTS, HEAD_SIZE)).astype(jnp.bfloat16)
    copies[1].wait()
    copies[2].wait()
    for i in range(groups):
        cut = pl.ds(pl.multiple_of((mine ^ i) * HEAD_SIZE, HEAD_SIZE), HEAD_SIZE)
        out[i][:rows, :] = k_buf[:, cut]
        out[i][rows : 2 * rows, :] = v_buf[:, cut]
        out[i][2 * rows :, :] = counts


def pack_queries(q_ref, *rest, groups):
    out, sems = rest[:groups], rest[groups]
    width = out[0].shape[1]
    mine = lax.axis_index("group")
    copies = []
    for i in range(groups):
        start = pl.multiple_of((mine ^ i) * width, width)
        copies.append(pltpu.make_async_copy(q_ref.at[:, pl.ds(start, width)], out[i], sems.at[i]))
        copies[-1].start()
    for copy in copies:
        copy.wait()


def merge(*refs, groups):
    pieces, out_ref = refs[:groups], refs[groups]
    mine = lax.axis_index("group")
    for i in range(groups):
        out_ref[mine ^ i] = pieces[i][...]


def attend(*refs, index, turns, rows, groups, layers, split, sides, resume, final):
    count = len(turns)
    q_ref, home_ref = refs[:2]
    refs = refs[2:]
    tiles = []
    for side in sides:
        tiles.append(refs[:count] if side else ())
        refs = refs[len(tiles[-1]) :]
    own, mate = tiles
    state, refs = (refs[:3], refs[3:]) if resume else (None, refs)
    out_ref, held = (refs[0], refs[1:]) if final else (None, refs)
    m_ref, l_ref, acc_ref, s_ref = held
    per = q_ref.shape[1] // HEAD_SIZE
    chips = home_ref.shape[0]
    scale = HEAD_SIZE ** -0.5 * LOG2E
    core, layer = lax.axis_index("core"), lax.axis_index("uly")
    home = lax.axis_index("outer") * groups + (lax.axis_index("group") ^ index)
    shape = (rows, HEAD_SIZE)
    lane = lax.broadcasted_iota(jnp.int32, (DOCUMENTS, HEAD_SIZE), 1).astype(jnp.float32)
    number = lax.broadcasted_iota(jnp.int32, (DOCUMENTS, HEAD_SIZE), 0).astype(jnp.float32)

    def counts(ref, chip):
        return ref[chip, 2 * rows :, :].astype(jnp.float32)

    mine = counts(home_ref, home)
    local_row = lax.broadcasted_iota(jnp.int32, shape, 0).astype(jnp.float32)
    row_doc = jnp.zeros(shape, jnp.float32)
    for d in range(DOCUMENTS):
        row_doc = row_doc + jnp.where(jnp.broadcast_to(mine[d : d + 1], shape) <= local_row, 1.0, 0.0)
    place = ((home * 2 + core) * layers + layer) * rows + lax.broadcasted_iota(jnp.int32, shape, 0)
    earliest = row_doc[:1] - 1.0

    def skipped(tiles):
        gone = jnp.zeros((1, HEAD_SIZE), jnp.float32)
        for chip in range(chips):
            least = None
            for ref in tiles:
                held_below = jnp.sum(jnp.where(number == earliest, counts(ref, chip), 0.0), axis=0, keepdims=True)
                least = held_below if least is None else jnp.minimum(least, held_below)
            gone = gone + jnp.where(least >= rows, 1.0, 0.0)
        return jnp.max(gone).astype(jnp.int32)

    m_ref[...] = jnp.full(m_ref.shape, LOW, jnp.float32)
    part = per // split
    heads = list(range(per))
    last_own, last_mate = home + 1, home + core
    first_own = skipped(own) if own else last_own
    first_mate = skipped(mate) if mate else last_mate
    second = last_own - first_own

    def strip(h):
        return pl.ds(h * rows, rows)

    def score(tiles, chip, parity, slot):
        k = jnp.concatenate([ref[chip, :rows, :] for ref in tiles], axis=0)
        bias = []
        for turn, ref in zip(turns, tiles):
            base = ((chip * 2 + parity) * layers + (layer ^ turn)) * rows
            key_doc = jnp.sum(jnp.where(counts(ref, chip) <= lane, 1.0, 0.0), axis=0, keepdims=True)
            key = base + lax.broadcasted_iota(jnp.int32, shape, 1)
            bias.append(jnp.where((key <= place) & (row_doc == key_doc), 0.0, LOW))
        for h0 in range(0, per, part):
            q = jnp.concatenate([q_ref[:, h * HEAD_SIZE : (h + 1) * HEAD_SIZE] for h in heads[h0 : h0 + part]], axis=0)
            s = lax.dot_general(q, k, (((1,), (1,)), ((), ())), preferred_element_type=jnp.float32)
            for i in range(part):
                xs = [s[i * rows : (i + 1) * rows, c * rows : (c + 1) * rows] + bias[c] for c in range(count)]
                for c in range(count):
                    s_ref[slot, strip(h0 + i), c * rows : (c + 1) * rows] = xs[c]
                m_ref[strip(h0 + i), :] = functools.reduce(jnp.maximum, xs, m_ref[strip(h0 + i), :])

    def weigh(tiles, chip, slot):
        v = jnp.concatenate([ref[chip, rows : 2 * rows, :] for ref in tiles], axis=0)
        for h0 in range(0, per, part):
            ps = []
            for h in heads[h0 : h0 + part]:
                shift = m_ref[strip(h), :]
                p = [
                    jnp.exp2(s_ref[slot, strip(h), c * rows : (c + 1) * rows] * scale - shift) for c in range(count)
                ]
                l_ref[strip(h), :] = functools.reduce(jnp.add, p, l_ref[strip(h), :])
                ps.append(jnp.concatenate([y.astype(jnp.bfloat16) for y in p], axis=1))
            pv = lax.dot_general(
                jnp.concatenate(ps, axis=0), v, (((1,), (0,)), ((), ())), preferred_element_type=jnp.float32
            )
            r = pl.ds(h0 * rows, part * rows)
            acc_ref[r, :] = acc_ref[r, :] + pv

    if own:

        @pl.loop(first_own, last_own)
        def _(chip):
            score(own, chip, core, chip - first_own)

    if mate:

        @pl.loop(first_mate, last_mate)
        def _(chip):
            score(mate, chip, 1 - core, second + chip - first_mate)

    for h in heads:
        r = strip(h)
        top = jnp.broadcast_to(jnp.max(m_ref[r, :], axis=1, keepdims=True) * scale, shape)
        if resume:
            old = state[0][r, :]
            top = jnp.maximum(top, old)
            factor = jnp.exp2(old - top)
            l_ref[r, :] = state[1][r, :] * factor
            acc_ref[r, :] = state[2][r, :] * factor
        else:
            l_ref[r, :] = jnp.zeros(shape, jnp.float32)
            acc_ref[r, :] = jnp.zeros(shape, jnp.float32)
        m_ref[r, :] = top

    if own:

        @pl.loop(first_own, last_own)
        def _(chip):
            weigh(own, chip, chip - first_own)

    if mate:

        @pl.loop(first_mate, last_mate)
        def _(chip):
            weigh(mate, chip, second + chip - first_mate)

    if final:
        for h in heads:
            r = strip(h)
            total = jnp.sum(l_ref[r, :], axis=1, keepdims=True)
            out_ref[:, h * HEAD_SIZE : (h + 1) * HEAD_SIZE] = (acc_ref[r, :] / total).astype(out_ref.dtype)


def place(*refs, groups):
    pieces, out_ref, sems = refs[:groups], refs[groups], refs[groups + 1]
    width = pieces[0].shape[1]
    mine = lax.axis_index("group")
    copies = []
    for i in range(groups):
        start = pl.multiple_of((mine ^ i) * width, width)
        copies.append(pltpu.make_async_copy(pieces[i], out_ref.at[:, pl.ds(start, width)], sems.at[i]))
        copies[-1].start()
    for copy in copies:
        copy.wait()


def limit(mib):
    return pltpu.CompilerParams(vmem_limit_bytes=mib << 20)


def local(queries, keys, values, segments, *, outer, groups, layers):
    rows = queries.shape[0]
    width = queries.shape[1] // groups
    per = width // HEAD_SIZE
    piece = jax.ShapeDtypeStruct((rows, width), jnp.bfloat16)
    one = jax.ShapeDtypeStruct((2 * rows + DOCUMENTS, HEAD_SIZE), jnp.bfloat16)
    raw = [pltpu.with_memory_space_constraint(x, pltpu.HBM) for x in (keys, values, segments.reshape(1, rows), queries)]
    kv = list(
        pl.pallas_call(
            functools.partial(pack, groups=groups),
            out_shape=[one] * groups,
            in_specs=[HBM] * 3,
            out_specs=[VMEM] * groups,
            scratch_shapes=[
                pltpu.VMEM(keys.shape, jnp.bfloat16),
                pltpu.VMEM(values.shape, jnp.bfloat16),
                pltpu.VMEM((1, rows), jnp.int32),
                pltpu.SemaphoreType.DMA((3,)),
            ],
            compiler_params=limit(4),
            name="pack",
        )(*raw[:3])
    )
    q = list(
        pl.pallas_call(
            functools.partial(pack_queries, groups=groups),
            out_shape=[piece] * groups,
            in_specs=[HBM],
            out_specs=[VMEM] * groups,
            scratch_shapes=[pltpu.SemaphoreType.DMA((groups,))],
            compiler_params=limit(4),
            name="pack_queries",
        )(raw[3])
    )

    def swap(x, axis, size, i):
        return lax.ppermute(x, axis, [(g, g ^ i) for g in range(size)])

    order = list(range(groups - 1, 0, -1))
    for i in order:
        kv[i] = swap(kv[i], "group", groups, i)
    for i in order:
        q[i] = swap(q[i], "group", groups, i)
    mine = pl.pallas_call(
        functools.partial(merge, groups=groups),
        out_shape=jax.ShapeDtypeStruct((groups, *one.shape), jnp.bfloat16),
        in_specs=[VMEM] * groups,
        out_specs=VMEM,
        compiler_params=limit(4),
        name="merge",
    )(*kv)
    if outer > 1:
        mine = lax.all_gather(mine, "outer", axis=0, tiled=True)
    own = [mine] + [swap(mine, "uly", layers, j) for j in range(1, layers)]
    mate = []
    for j in range(layers):
        mate.append(lax.ppermute(own[j], "core", [(0, 1), (1, 0)]))

    held = [jax.ShapeDtypeStruct((per * rows, HEAD_SIZE), jnp.float32)] * 3
    common = dict(rows=rows, groups=groups, layers=layers, split=1)
    units = 2 * (outer * groups // 2 + 1)
    near, far = list(range(layers // 2)), list(range(layers // 2, layers))

    def call(i, turns, sides, state, final):
        args = [q[i], own[0]]
        for side, held_by in zip(sides, (own, mate)):
            args += [held_by[j] for j in turns] if side else []
        args += state or []
        keep = dict(sides=sides, resume=state is not None, final=final)
        return pl.pallas_call(
            functools.partial(attend, index=i, turns=turns, **keep, **common),
            out_shape=piece if final else held,
            in_specs=[VMEM] * len(args),
            out_specs=VMEM if final else [VMEM] * 3,
            scratch_shapes=([pltpu.VMEM(x.shape, x.dtype) for x in held] if final else [])
            + [pltpu.VMEM((units, per * rows, len(turns) * rows), jnp.float32)],
            compiler_params=limit(8 + units),
            name="attend",
        )(*args)

    both, states, out, last = (True, True), [None] * groups, [None] * groups, None

    def follow(i):
        nonlocal last
        if last is not None:
            q[i], last = lax.optimization_barrier((q[i], last))

    for i in [0] + order:
        follow(i)
        states[i] = call(i, near, both, None, False)
        last = states[i][0]
    i = order[0]
    follow(i)
    states[i] = call(i, far, (True, False), states[i], False)
    last = states[i][0]
    for i in order + [0]:
        follow(i)
        last = call(i, far, (False, True) if i == order[0] else both, states[i], True)
        out[i] = swap(last, "group", groups, i) if i else last
    return pl.pallas_call(
        functools.partial(place, groups=groups),
        out_shape=jax.ShapeDtypeStruct(queries.shape, jnp.bfloat16),
        in_specs=[VMEM] * groups,
        out_specs=HBM,
        scratch_shapes=[pltpu.SemaphoreType.DMA((groups,))],
        compiler_params=limit(4),
        name="place",
    )(*out)


def solution(mesh):
    blocks, layers = mesh.shape["blk"], mesh.shape["uly"]

    def run(queries, keys, values, segments):
        groups = keys.shape[1] // HEAD_SIZE
        outer = blocks // 2 // groups
        fine = Mesh(mesh.devices.reshape(outer, groups, 2, layers), AXES)

        def body(*args):
            return local(*args, outer=outer, groups=groups, layers=layers)

        spec = P(AXES)
        step = jax.shard_map(body, mesh=fine, in_specs=(spec,) * 4, out_specs=spec, check_vma=False)
        return step(queries, keys, values, segments)

    return run
```

```python
import functools

import jax
import jax.numpy as jnp
from jax import lax
from jax.experimental import pallas as pl
from jax.experimental.pallas import tpu as pltpu
from jax.sharding import Mesh
from jax.sharding import PartitionSpec as P


HEAD_SIZE = 128
DOCUMENTS = 8
LOG2E = 1.4426950408889634
LOW = -1e30
AXES = ("outer", "group", "core", "uly")
VMEM = pl.BlockSpec(memory_space=pltpu.VMEM)
HBM = pl.BlockSpec(memory_space=pltpu.HBM)


def pack(k_ref, v_ref, seg_ref, *rest, groups):
    out, (k_buf, v_buf, seg_buf, sems) = rest[:groups], rest[groups:]
    rows = k_buf.shape[0]
    mine = lax.axis_index("group")
    pairs = ((seg_ref, seg_buf), (k_ref, k_buf), (v_ref, v_buf))
    copies = [pltpu.make_async_copy(x, y, sems.at[i]) for i, (x, y) in enumerate(pairs)]
    for copy in copies:
        copy.start()
    copies[0].wait()
    number = lax.broadcasted_iota(jnp.int32, (DOCUMENTS, rows), 0)
    below = jnp.where(seg_buf[...] < number, 1.0, 0.0)
    counts = jnp.broadcast_to(jnp.sum(below, axis=1, keepdims=True), (DOCUMENTS, HEAD_SIZE)).astype(jnp.bfloat16)
    copies[1].wait()
    copies[2].wait()
    for i in range(groups):
        cut = pl.ds(pl.multiple_of((mine ^ i) * HEAD_SIZE, HEAD_SIZE), HEAD_SIZE)
        out[i][:rows, :] = k_buf[:, cut]
        out[i][rows : 2 * rows, :] = v_buf[:, cut]
        out[i][2 * rows :, :] = counts


def pack_queries(q_ref, *rest, groups):
    out, sems = rest[:groups], rest[groups]
    width = out[0].shape[1]
    mine = lax.axis_index("group")
    copies = []
    for i in range(groups):
        start = pl.multiple_of((mine ^ i) * width, width)
        copies.append(pltpu.make_async_copy(q_ref.at[:, pl.ds(start, width)], out[i], sems.at[i]))
        copies[-1].start()
    for copy in copies:
        copy.wait()


def merge(*refs, groups):
    pieces, out_ref = refs[:groups], refs[groups]
    mine = lax.axis_index("group")
    for i in range(groups):
        out_ref[mine ^ i] = pieces[i][...]


def attend(*refs, index, turns, rows, groups, layers, split, sides, resume, final):
    count = len(turns)
    q_ref, home_ref = refs[:2]
    refs = refs[2:]
    tiles = []
    for side in sides:
        tiles.append(refs[:count] if side else ())
        refs = refs[len(tiles[-1]) :]
    own, mate = tiles
    state, refs = (refs[:3], refs[3:]) if resume else (None, refs)
    out_ref, held = (refs[0], refs[1:]) if final else (None, refs)
    m_ref, l_ref, acc_ref, s_ref = held
    per = q_ref.shape[1] // HEAD_SIZE
    chips = home_ref.shape[0]
    scale = HEAD_SIZE ** -0.5 * LOG2E
    core, layer = lax.axis_index("core"), lax.axis_index("uly")
    home = lax.axis_index("outer") * groups + (lax.axis_index("group") ^ index)
    shape = (rows, HEAD_SIZE)
    lane = lax.broadcasted_iota(jnp.int32, (DOCUMENTS, HEAD_SIZE), 1).astype(jnp.float32)
    number = lax.broadcasted_iota(jnp.int32, (DOCUMENTS, HEAD_SIZE), 0).astype(jnp.float32)

    def counts(ref, chip):
        return ref[chip, 2 * rows :, :].astype(jnp.float32)

    mine = counts(home_ref, home)
    local_row = lax.broadcasted_iota(jnp.int32, shape, 0).astype(jnp.float32)
    row_doc = jnp.zeros(shape, jnp.float32)
    for d in range(DOCUMENTS):
        row_doc = row_doc + jnp.where(jnp.broadcast_to(mine[d : d + 1], shape) <= local_row, 1.0, 0.0)
    place = ((home * 2 + core) * layers + layer) * rows + lax.broadcasted_iota(jnp.int32, shape, 0)
    earliest = row_doc[:1] - 1.0

    def skipped(tiles):
        gone = jnp.zeros((1, HEAD_SIZE), jnp.float32)
        for chip in range(chips):
            least = None
            for ref in tiles:
                held_below = jnp.sum(jnp.where(number == earliest, counts(ref, chip), 0.0), axis=0, keepdims=True)
                least = held_below if least is None else jnp.minimum(least, held_below)
            gone = gone + jnp.where(least >= rows, 1.0, 0.0)
        return jnp.max(gone).astype(jnp.int32)

    m_ref[...] = jnp.full(m_ref.shape, LOW, jnp.float32)
    part = per // split
    heads = list(range(per))
    earlier = functools.reduce(jnp.logical_or, [(layer ^ turn) <= layer for turn in turns])
    last_own, last_mate = home + jnp.where(earlier, 1, 0), home + core
    first_own = skipped(own) if own else last_own
    first_mate = skipped(mate) if mate else last_mate
    second = jnp.maximum(last_own - first_own, 0)

    def strip(h):
        return pl.ds(h * rows, rows)

    def score(tiles, chip, parity, slot):
        k = jnp.concatenate([ref[chip, :rows, :] for ref in tiles], axis=0)
        bias = []
        for turn, ref in zip(turns, tiles):
            base = ((chip * 2 + parity) * layers + (layer ^ turn)) * rows
            key_doc = jnp.sum(jnp.where(counts(ref, chip) <= lane, 1.0, 0.0), axis=0, keepdims=True)
            key = base + lax.broadcasted_iota(jnp.int32, shape, 1)
            bias.append(jnp.where((key <= place) & (row_doc == key_doc), 0.0, LOW))
        for h0 in range(0, per, part):
            q = jnp.concatenate([q_ref[:, h * HEAD_SIZE : (h + 1) * HEAD_SIZE] for h in heads[h0 : h0 + part]], axis=0)
            s = lax.dot_general(q, k, (((1,), (1,)), ((), ())), preferred_element_type=jnp.float32)
            for i in range(part):
                xs = [s[i * rows : (i + 1) * rows, c * rows : (c + 1) * rows] + bias[c] for c in range(count)]
                for c in range(count):
                    s_ref[slot, strip(h0 + i), c * rows : (c + 1) * rows] = xs[c]
                m_ref[strip(h0 + i), :] = functools.reduce(jnp.maximum, xs, m_ref[strip(h0 + i), :])

    def weigh(tiles, chip, slot):
        v = jnp.concatenate([ref[chip, rows : 2 * rows, :] for ref in tiles], axis=0)
        for h0 in range(0, per, part):
            ps = []
            for h in heads[h0 : h0 + part]:
                shift = m_ref[strip(h), :]
                p = [
                    jnp.exp2(s_ref[slot, strip(h), c * rows : (c + 1) * rows] * scale - shift) for c in range(count)
                ]
                l_ref[strip(h), :] = functools.reduce(jnp.add, p, l_ref[strip(h), :])
                ps.append(jnp.concatenate([y.astype(jnp.bfloat16) for y in p], axis=1))
            pv = lax.dot_general(
                jnp.concatenate(ps, axis=0), v, (((1,), (0,)), ((), ())), preferred_element_type=jnp.float32
            )
            r = pl.ds(h0 * rows, part * rows)
            acc_ref[r, :] = acc_ref[r, :] + pv

    if own:

        @pl.loop(first_own, last_own)
        def _(chip):
            score(own, chip, core, chip - first_own)

    if mate:

        @pl.loop(first_mate, last_mate)
        def _(chip):
            score(mate, chip, 1 - core, second + chip - first_mate)

    for h in heads:
        r = strip(h)
        top = jnp.broadcast_to(jnp.max(m_ref[r, :], axis=1, keepdims=True) * scale, shape)
        if resume:
            old = state[0][r, :]
            top = jnp.maximum(top, old)
            factor = jnp.exp2(old - top)
            l_ref[r, :] = state[1][r, :] * factor
            acc_ref[r, :] = state[2][r, :] * factor
        else:
            l_ref[r, :] = jnp.zeros(shape, jnp.float32)
            acc_ref[r, :] = jnp.zeros(shape, jnp.float32)
        m_ref[r, :] = top

    if own:

        @pl.loop(first_own, last_own)
        def _(chip):
            weigh(own, chip, chip - first_own)

    if mate:

        @pl.loop(first_mate, last_mate)
        def _(chip):
            weigh(mate, chip, second + chip - first_mate)

    if final:
        for h in heads:
            r = strip(h)
            total = jnp.sum(l_ref[r, :], axis=1, keepdims=True)
            out_ref[:, h * HEAD_SIZE : (h + 1) * HEAD_SIZE] = (acc_ref[r, :] / total).astype(out_ref.dtype)


def place(*refs, groups):
    pieces, out_ref, sems = refs[:groups], refs[groups], refs[groups + 1]
    width = pieces[0].shape[1]
    mine = lax.axis_index("group")
    copies = []
    for i in range(groups):
        start = pl.multiple_of((mine ^ i) * width, width)
        copies.append(pltpu.make_async_copy(pieces[i], out_ref.at[:, pl.ds(start, width)], sems.at[i]))
        copies[-1].start()
    for copy in copies:
        copy.wait()


def limit(mib):
    return pltpu.CompilerParams(vmem_limit_bytes=mib << 20)


def local(queries, keys, values, segments, *, outer, groups, layers):
    rows = queries.shape[0]
    width = queries.shape[1] // groups
    per = width // HEAD_SIZE
    piece = jax.ShapeDtypeStruct((rows, width), jnp.bfloat16)
    one = jax.ShapeDtypeStruct((2 * rows + DOCUMENTS, HEAD_SIZE), jnp.bfloat16)
    raw = [pltpu.with_memory_space_constraint(x, pltpu.HBM) for x in (keys, values, segments.reshape(1, rows), queries)]
    kv = list(
        pl.pallas_call(
            functools.partial(pack, groups=groups),
            out_shape=[one] * groups,
            in_specs=[HBM] * 3,
            out_specs=[VMEM] * groups,
            scratch_shapes=[
                pltpu.VMEM(keys.shape, jnp.bfloat16),
                pltpu.VMEM(values.shape, jnp.bfloat16),
                pltpu.VMEM((1, rows), jnp.int32),
                pltpu.SemaphoreType.DMA((3,)),
            ],
            compiler_params=limit(4),
            name="pack",
        )(*raw[:3])
    )
    q = list(
        pl.pallas_call(
            functools.partial(pack_queries, groups=groups),
            out_shape=[piece] * groups,
            in_specs=[HBM],
            out_specs=[VMEM] * groups,
            scratch_shapes=[pltpu.SemaphoreType.DMA((groups,))],
            compiler_params=limit(4),
            name="pack_queries",
        )(raw[3])
    )

    def swap(x, axis, size, i):
        return lax.ppermute(x, axis, [(g, g ^ i) for g in range(size)])

    order = list(range(groups - 1, 0, -1))
    for i in order:
        kv[i] = swap(kv[i], "group", groups, i)
    for i in order:
        q[i] = swap(q[i], "group", groups, i)
    mine = pl.pallas_call(
        functools.partial(merge, groups=groups),
        out_shape=jax.ShapeDtypeStruct((groups, *one.shape), jnp.bfloat16),
        in_specs=[VMEM] * groups,
        out_specs=VMEM,
        compiler_params=limit(4),
        name="merge",
    )(*kv)
    if outer > 1:
        mine = lax.all_gather(mine, "outer", axis=0, tiled=True)
    own = [mine] + [swap(mine, "uly", layers, j) for j in range(1, layers)]
    mate = []
    for j in range(layers):
        mate.append(lax.ppermute(own[j], "core", [(0, 1), (1, 0)]))

    held = [jax.ShapeDtypeStruct((per * rows, HEAD_SIZE), jnp.float32)] * 3
    common = dict(rows=rows, groups=groups, layers=layers, split=2)
    units = 2 * (outer * groups // 2 + 1)
    near, far = list(range(layers // 2)), list(range(layers // 2, layers))

    def call(i, turns, sides, state, final):
        args = [q[i], own[0]]
        for side, held_by in zip(sides, (own, mate)):
            args += [held_by[j] for j in turns] if side else []
        args += state or []
        keep = dict(sides=sides, resume=state is not None, final=final)
        return pl.pallas_call(
            functools.partial(attend, index=i, turns=turns, **keep, **common),
            out_shape=piece if final else held,
            in_specs=[VMEM] * len(args),
            out_specs=VMEM if final else [VMEM] * 3,
            scratch_shapes=([pltpu.VMEM(x.shape, x.dtype) for x in held] if final else [])
            + [pltpu.VMEM((units, per * rows, len(turns) * rows), jnp.float32)],
            compiler_params=limit(8 + units),
            name="attend",
        )(*args)

    both, states, out, last = (True, True), [None] * groups, [None] * groups, None

    def follow(i):
        nonlocal last
        if last is not None:
            q[i], last = lax.optimization_barrier((q[i], last))

    for i in [0] + order:
        follow(i)
        states[i] = call(i, near, both, None, False)
        last = states[i][0]
    i = order[0]
    follow(i)
    states[i] = call(i, far, (True, False), states[i], False)
    last = states[i][0]
    for i in order + [0]:
        follow(i)
        last = call(i, far, (False, True) if i == order[0] else both, states[i], True)
        out[i] = swap(last, "group", groups, i) if i else last
    return pl.pallas_call(
        functools.partial(place, groups=groups),
        out_shape=jax.ShapeDtypeStruct(queries.shape, jnp.bfloat16),
        in_specs=[VMEM] * groups,
        out_specs=HBM,
        scratch_shapes=[pltpu.SemaphoreType.DMA((groups,))],
        compiler_params=limit(4),
        name="place",
    )(*out)


def solution(mesh):
    blocks, layers = mesh.shape["blk"], mesh.shape["uly"]

    def run(queries, keys, values, segments):
        groups = keys.shape[1] // HEAD_SIZE
        outer = blocks // 2 // groups
        fine = Mesh(mesh.devices.reshape(outer, groups, 2, layers), AXES)

        def body(*args):
            return local(*args, outer=outer, groups=groups, layers=layers)

        spec = P(AXES)
        step = jax.shard_map(body, mesh=fine, in_specs=(spec,) * 4, out_specs=spec, check_vma=False)
        return step(queries, keys, values, segments)

    return run
```
